16 devices in a mesh: dp: 1, ep: 16 (over x, y, z, core).
Axes of the slice: x: 2, y: 2, z: 2, core: 2. Of those that a mesh axis runs over, the one named last changes fastest.
Arguments:
- x: bfloat16 [1, 16, 256, 4096], P('dp', 'ep')
- expert: int32 [1, 16, 256, 8], P('dp', 'ep')
- slot: int32 [1, 16, 256, 8], P('dp', 'ep')
- gate: float32 [1, 16, 256, 8], P('dp', 'ep')
- w_gate: bfloat16 [64, 4096, 1408], P('ep')
- w_up: bfloat16 [64, 4096, 1408], P('ep')
- w_down: bfloat16 [64, 1408, 4096], P('ep')
- s_gate: bfloat16 [4096, 1408], replicated
- s_up: bfloat16 [4096, 1408], replicated
- s_down: bfloat16 [1408, 4096], replicated
Outputs:
- y: bfloat16 [1, 16, 256, 4096], P('dp', 'ep')
All inputs are finite; a program needn't handle non-finite values.
Results may differ from the reference program's by a relative error of at most 0.009.
Values are sent between devices in bfloat16 or wider.
A program may use at most 2 GiB of HBM per device.

```python
import jax
import jax.numpy as jnp

MEMBERS = 16
TOKENS = 256
D = 4096
FF = 1408
TOP = 8
EXPERTS = 64
SHARED_FF = 1408
SLOTS = 5 * TOKENS * TOP // (4 * EXPERTS)


def setup_inputs(seed: int = 0, part: int = 0) -> dict:
    own, k1, k2, k3, k4, k5, k6 = jax.random.split(jax.random.key(seed), 7)
    kx, ke, kl, kg = jax.random.split(jax.random.fold_in(own, part), 4)
    devices = (1, MEMBERS)
    place = jax.random.permutation(kl, jnp.arange(EXPERTS, dtype=jnp.uint32))
    slow = ((EXPERTS + (9 * place) % EXPERTS) << ((9 * place) // EXPERTS)) // EXPERTS
    wait = (jax.random.bits(ke, (*devices, TOKENS, EXPERTS), jnp.uint32) >> 10) * slow
    expert = jnp.argsort(wait, axis=-1)[..., :TOP].astype(jnp.int32)
    chosen = jax.nn.one_hot(expert, EXPERTS, dtype=jnp.int32)
    in_line = jnp.cumsum(chosen.reshape(*devices, TOKENS * TOP, EXPERTS), axis=2) - 1
    slot = jnp.sum(in_line.reshape(chosen.shape) * chosen, axis=-1)

    def one(key, rows, columns):
        return (jax.random.normal(key, (rows, columns), jnp.float32) * rows**-0.5).astype(jnp.bfloat16)

    def weights(key, rows, columns):
        return jax.lax.map(lambda k: one(k, rows, columns), jax.random.split(key, EXPERTS))

    return {
        "x": jax.random.normal(kx, (*devices, TOKENS, D), jnp.float32).astype(jnp.bfloat16),
        "expert": expert,
        "slot": slot,
        "gate": jax.nn.softmax(jax.random.normal(kg, expert.shape, jnp.float32)),
        "w_gate": weights(k1, D, FF),
        "w_up": weights(k2, D, FF),
        "w_down": weights(k3, FF, D),
        "s_gate": one(k4, D, SHARED_FF),
        "s_up": one(k5, D, SHARED_FF),
        "s_down": one(k6, SHARED_FF, D),
    }


def einsum(form, a, b):
    return jnp.einsum(form, a.astype(jnp.float32), b.astype(jnp.float32))


def for_all(x, s_gate, s_up, s_down):
    h = jax.nn.silu(einsum("...d,df->...f", x, s_gate)) * einsum("...d,df->...f", x, s_up)
    return einsum("...f,fd->...d", h.astype(jnp.bfloat16), s_down)


def reference(x, expert, slot, gate, w_gate, w_up, w_down, s_gate, s_up, s_down):
    to_expert = jax.nn.one_hot(expert, EXPERTS, dtype=jnp.bfloat16)
    to_slot = jax.nn.one_hot(slot, SLOTS, dtype=jnp.bfloat16)
    weighted = to_expert * gate[..., None].astype(jnp.bfloat16)
    dispatch = einsum("abtke,abtkc->abtec", to_expert, to_slot).astype(jnp.bfloat16)
    combine = einsum("abtke,abtkc->abtec", weighted, to_slot).astype(jnp.bfloat16)
    z = einsum("abtec,abtd->aebcd", dispatch, x).astype(jnp.bfloat16)
    h = jax.nn.silu(einsum("aebcd,edf->aebcf", z, w_gate))
    h = (h * einsum("aebcd,edf->aebcf", z, w_up)).astype(jnp.bfloat16)
    out = einsum("aebcf,efd->aebcd", h, w_down).astype(jnp.bfloat16)
    y = einsum("abtec,aebcd->abtd", combine, out)
    return (y + for_all(x, s_gate, s_up, s_down)).astype(jnp.bfloat16)
```

```python
import functools

import jax
import jax.numpy as jnp
from jax import lax
from jax.experimental import pallas as pl
from jax.experimental.pallas import tpu as pltpu
from jax.sharding import PartitionSpec as P

MESH = pl.DeviceIdType.MESH
DK = 512
PARTS = ((0, 96), (96, 80), (176, 80))
LIMIT = 67_000_000
F32, BF16 = jnp.float32, jnp.bfloat16


class Place:
    def __init__(self):
        self.me = lax.axis_index("ep")
        self.bits = [lax.rem(lax.div(self.me, m), 2) for m in (8, 4, 2)]
        self.core = lax.rem(self.me, 2)
        self.partner = self.me + 1 - 2 * self.core

    def across(self, d):
        ids = [self.me + m * (1 - 2 * b) for m, b in zip((8, 4, 2), self.bits)]
        return ids[0] * lax.div((1 - d) * (2 - d), 2) + ids[1] * (d * (2 - d)) + ids[2] * lax.div(d * (d - 1), 2)

    def chip(self, m):
        ms = (lax.div(m, 4), lax.rem(lax.div(m, 2), 2), lax.rem(m, 2))
        x, y, z = (b + s * (1 - 2 * b) for b, s in zip(self.bits, ms))
        return ((x * 2 + y) * 2 + z) * 2


def turn(o, i):
    return lax.rem(o + i, 3)


def chip_at(o, pos):
    m = 0
    for i in range(3):
        if pos >> i & 1:
            d = turn(o, i)
            m = m + 4 - 2 * d + lax.div(d * (d - 1), 2)
    return m


def cols(k, width=DK):
    return pl.ds(pl.multiple_of(k * width, width), width)


def gather_kernel(
    x, route, wg, wu, sg, su,
    h_out, hs_out, g_out, r0, r1, r2, q0, q1, q2,
    rt, xv, z, wbuf, acc, accs, sbuf, gbuf, hbuf,
    route_send, route_recv, fill, send, recv1, recv2, recv3, drecv, load, wsem, gsem, hsem,
):
    at = Place()
    me = at.me
    tokens, d_model = x.shape
    chunks = d_model // DK
    experts, slots = 4, 40
    ff = wg.shape[2]
    r, q = (r0, r1, r2), (q0, q1, q2)

    def remote(src, dst, s, v, dev):
        return pltpu.make_async_remote_copy(
            src_ref=src, dst_ref=dst, send_sem=s, recv_sem=v, device_id={"ep": dev}, device_id_type=MESH
        )

    def first(k, p):
        row, size = PARTS[p]
        return remote(x.at[pl.ds(row, size), cols(k)], r[p].at[k, 1], send.at[0, p], recv1.at[p, k], at.across(turn(k, p)))

    def second(k, p):
        return remote(
            r[p].at[k, pl.ds(0, 2)], r[p].at[k, pl.ds(2, 2)], send.at[1, p], recv2.at[p, k], at.across(turn(k, p + 1))
        )

    def third(k, p):
        return remote(
            r[p].at[k, pl.ds(0, 4)], r[p].at[k, pl.ds(4, 4)], send.at[2, p], recv3.at[p, k], at.across(turn(k, p + 2))
        )

    def beside(k, p, i):
        half = pl.ds(4 * i, 4)
        return remote(r[p].at[k, half], q[p].at[k, half], send.at[3 + i, p], drecv.at[i, p, k], at.partner)

    def filled(k, p):
        row, size = PARTS[p]
        return pltpu.make_async_copy(x.at[pl.ds(row, size), cols(k)], r[p].at[k, 0], fill.at[p, k])

    def weights(i):
        slot = lax.rem(i, 3)
        left, right = wbuf.at[slot, :, pl.ds(0, ff)], wbuf.at[slot, :, pl.ds(ff, ff)]

        @pl.when(i < chunks)
        def _():
            rows = cols(i)
            pltpu.make_async_copy(sg.at[rows], left, wsem.at[slot]).start()
            pltpu.make_async_copy(su.at[rows], right, wsem.at[slot]).start()

        @pl.when(jnp.logical_and(i >= chunks, i < 5 * chunks))
        def _():
            j = i - chunks
            e, rows = lax.rem(j, 4), cols(lax.div(j, 4))
            pltpu.make_async_copy(wg.at[e, rows], left, wsem.at[slot]).start()
            pltpu.make_async_copy(wu.at[e, rows], right, wsem.at[slot]).start()

    def weights_ready(i):
        slot = lax.rem(i, 3)
        pltpu.make_async_copy(wbuf.at[slot], wbuf.at[slot], wsem.at[slot]).wait()
        weights(i + 2)
        return slot

    def load_rows(k, src, core, i):
        slot = lax.rem(k, 2)
        for p, (row, size) in enumerate(PARTS):
            o = turn(k, p)
            for pos in range(8):
                dst = xv.at[slot, chip_at(o, pos), pl.ds(pl.multiple_of(core * tokens + row, 16), size)]
                pltpu.make_async_copy(src[p].at[k, pos], dst, load.at[slot, i]).start()

    def rows_ready(k, i):
        slot = lax.rem(k, 2)
        half = xv.at[slot, :, pl.ds(0, tokens)]
        pltpu.make_async_copy(half, half, load.at[slot, i]).wait()

    weights(0)
    weights(1)
    for j in range(1, 16):
        dev = lax.rem(me + j, 16)
        remote(route, rt.at[me], route_send, route_recv.at[me], dev).start()
    rt[me] = route[...]
    for k in range(chunks):
        for p in range(3):
            filled(k, p).start()

    def build(m):
        base = at.chip(m)
        slot_of = lax.broadcasted_iota(jnp.int32, (80, tokens), 0)
        other = slot_of >= slots
        slot_of = jnp.where(other, slot_of - slots, slot_of)

        @pl.when(m >= 1)
        def _():
            pltpu.make_async_copy(gbuf, g_out.at[m - 1], gsem).wait()

        def one(e, _):
            want = (slot_of + (me * experts + e) * slots).astype(F32)
            rows = pl.ds(pl.multiple_of(e * 80, 80), 80)
            for c in range(2):
                here = jnp.where(other == (c == 1), want, -2.0)
                table = rt[base + c]
                s = jnp.zeros((80, tokens), F32)
                g = jnp.zeros((80, tokens), F32)
                for j in range(8):
                    hit = here == table[j : j + 1]
                    s = jnp.where(hit, 1.0, s)
                    g = jnp.where(hit, table[8 + j : 9 + j], g)
                sbuf[m, rows, c * tokens : (c + 1) * tokens] = s.astype(BF16)
                gbuf[rows, c * tokens : (c + 1) * tokens] = g.astype(BF16)
            return 0

        lax.fori_loop(0, experts, one, 0)
        pltpu.make_async_copy(gbuf, g_out.at[m], gsem).start()

    def clear(e, _):
        acc[e] = jnp.zeros(acc.shape[1:], F32)
        return 0

    def shared(i):
        slot = weights_ready(i)

        def tile(j, _):
            c = cols(j, 256)
            accs[:, c] += jnp.dot(x[:, cols(i)], wbuf[slot, :, c], preferred_element_type=F32)
            return 0

        lax.fori_loop(0, 2 * ff // 256, tile, 0)

    def compute(k):
        slot = lax.rem(k, 2)

        def dispatch(m, _):
            d = jnp.dot(sbuf[m], xv[slot, m], preferred_element_type=F32).astype(BF16)
            rows = pl.ds(pl.multiple_of(m * 80, 80), 80)
            for e in range(experts):
                z[e, rows] = d[e * 80 : (e + 1) * 80]
            return 0

        lax.fori_loop(0, 8, dispatch, 0)

        def expert(e, _):
            wslot = weights_ready(chunks + 4 * k + e)

            def tile(j, _):
                c = cols(j, 256)
                acc[e, :, c] += jnp.dot(z[e], wbuf[wslot, :, c], preferred_element_type=F32)
                return 0

            return lax.fori_loop(0, 2 * ff // 256, tile, 0)

        lax.fori_loop(0, experts, expert, 0)

    def step(s, _):
        @pl.when(s < chunks)
        def _():
            for p in range(3):
                first(s, p).start()

        @pl.when(jnp.logical_and(s >= 1, s < chunks + 1))
        def _():
            k = s - 1
            for p in range(3):
                filled(k, p).wait()
                first(k, p).wait_recv()
                second(k, p).start()

        @pl.when(jnp.logical_and(s >= 2, s < chunks + 2))
        def _():
            k = s - 2
            for p in range(3):
                second(k, p).wait_recv()
                third(k, p).start()
                beside(k, p, 0).start()

        @pl.when(s == 0)
        def _():
            accs[...] = jnp.zeros(accs.shape, F32)

        @pl.when(s < 4)
        def _():
            clear(s, 0)
            shared(2 * s)
            shared(2 * s + 1)

        @pl.when(s == 2)
        def _():
            for j in range(1, 16):
                b = lax.rem(me + j, 16)
                remote(route, rt.at[b], route_send, route_recv.at[b], b).wait_recv()

            def one(m, _):
                build(m)
                return 0

            lax.fori_loop(0, 8, one, 0)
            pltpu.make_async_copy(gbuf, g_out.at[7], gsem).wait()

        @pl.when(jnp.logical_and(s >= 3, s < chunks + 3))
        def _():
            k = s - 3
            for p in range(3):
                third(k, p).wait_recv()
                beside(k, p, 1).start()
            load_rows(k, r, at.core, 0)

        @pl.when(s >= 4)
        def _():
            k = s - 4
            for p in range(3):
                beside(k, p, 0).wait_recv()
                beside(k, p, 1).wait_recv()
            load_rows(k, q, 1 - at.core, 1)
            rows_ready(k, 0)
            rows_ready(k, 1)
            compute(k)

        return 0

    lax.fori_loop(0, chunks + 4, step, 0)

    def hidden(src, dst, i, rows):
        slot = lax.rem(i, 2)

        @pl.when(i >= 2)
        def _():
            pltpu.make_async_copy(hbuf.at[slot], dst, hsem.at[slot]).wait()

        a = src[rows, pl.ds(0, ff)]
        hbuf[slot] = (a * jax.nn.sigmoid(a) * src[rows, pl.ds(ff, ff)]).astype(BF16)
        pltpu.make_async_copy(hbuf.at[slot], dst, hsem.at[slot]).start()

    def routed(i, _):
        e, rows = lax.div(i, 10), pl.ds(pl.multiple_of(lax.rem(i, 10) * 64, 64), 64)
        hidden(acc.at[e], h_out.at[e, rows], i, rows)
        return 0

    lax.fori_loop(0, 10 * experts, routed, 0)

    def common(i, _):
        rows = pl.ds(pl.multiple_of(i * 64, 64), 64)
        hidden(accs, hs_out.at[rows], i + 10 * experts, rows)
        return 0

    lax.fori_loop(0, tokens // 64, common, 0)
    for slot in range(2):
        pltpu.make_async_copy(hbuf.at[slot], hs_out.at[pl.ds(0, 64)], hsem.at[slot]).wait()

    remote(rt.at[pl.ds(0, 15)], rt.at[pl.ds(0, 15)], route_send, route_recv.at[0], at.partner).wait_send()
    for p in range(3):
        one, two, four, rest = r[p].at[:, 0], r[p].at[:, pl.ds(0, 2)], r[p].at[:, pl.ds(0, 4)], r[p].at[:, pl.ds(4, 4)]
        for i, sent in enumerate((one, two, four, four, rest)):
            remote(sent, sent, send.at[i, p], recv1.at[p, 0], at.partner).wait_send()


def scatter_kernel(
    h, hs, g, wd, sd,
    y,
    hv, hsv, gv, wbuf, o, dsend, dland, acc8, acc4, acc2, acc1,
    as0, as1, as2, bs0, bs1, bs2, cs0, cs1, cs2,
    al0, al1, al2, bl0, bl1, bl2, cl0, cl1, cl2,
    start_sem, wsem, dsend_sem, drecv, free, asend_sem, bsend_sem, csend_sem, arecv, brecv, crecv,
):
    at = Place()
    tokens, d_model = y.shape
    chunks = d_model // DK
    experts = h.shape[0]
    ff = h.shape[2]
    a_send, b_send, c_send = (as0, as1, as2), (bs0, bs1, bs2), (cs0, cs1, cs2)
    a_land, b_land, c_land = (al0, al1, al2), (bl0, bl1, bl2), (cl0, cl1, cl2)

    def remote(src, dst, s, v, dev):
        return pltpu.make_async_remote_copy(
            src_ref=src, dst_ref=dst, send_sem=s, recv_sem=v, device_id={"ep": dev}, device_id_type=MESH
        )

    def beside(k):
        slot = lax.rem(k, 2)
        return remote(dsend.at[slot], dland.at[slot], dsend_sem.at[slot], drecv.at[slot], at.partner)

    def hop(stage, k, p):
        slot = lax.rem(k, 2)
        src, dst = (a_send, b_send, c_send)[stage][p], (a_land, b_land, c_land)[stage][p]
        sems, lands = (asend_sem, bsend_sem, csend_sem)[stage], (arecv, brecv, crecv)[stage]
        return remote(src.at[slot], dst.at[k], sems.at[p, slot], lands.at[p, k], at.across(turn(k, p + 2 - stage)))

    def weights(i):
        slot = lax.rem(i, 3)
        k, e = lax.div(i, 5), lax.rem(i, 5)

        @pl.when(jnp.logical_and(i < 5 * chunks, e < 4))
        def _():
            pltpu.make_async_copy(wd.at[e, :, cols(k)], wbuf.at[slot], wsem.at[slot]).start()

        @pl.when(jnp.logical_and(i < 5 * chunks, e == 4))
        def _():
            pltpu.make_async_copy(sd.at[:, cols(k)], wbuf.at[slot], wsem.at[slot]).start()

    def weights_ready(i):
        slot = lax.rem(i, 3)
        pltpu.make_async_copy(wbuf.at[slot], wbuf.at[slot], wsem.at[slot]).wait()
        weights(i + 2)
        return slot

    begin = [
        pltpu.make_async_copy(h, hv, start_sem.at[0]),
        pltpu.make_async_copy(hs, hsv, start_sem.at[1]),
        pltpu.make_async_copy(g, gv, start_sem.at[2]),
    ]
    weights(0)
    for copy in begin:
        copy.start()
    weights(1)
    for copy in begin:
        copy.wait()

    def compute(k):
        slot = lax.rem(k, 2)

        def expert(e, _):
            wslot = weights_ready(5 * k + e)

            def tile(j, _):
                c = cols(j, 256)
                o[e, :, c] = jnp.dot(hv[e], wbuf[wslot, :, c], preferred_element_type=F32).astype(BF16)
                return 0

            return lax.fori_loop(0, DK // 256, tile, 0)

        lax.fori_loop(0, experts, expert, 0)

        @pl.when(k >= 2)
        def _():
            beside(k).wait_send()

        def combine(m, _):
            rows = o[:, pl.ds(pl.multiple_of(m * 80, 80), 80), :].reshape(4 * 80, DK)
            mine = gv[m, :, cols(at.core, 256)]
            theirs = gv[m, :, cols(1 - at.core, 256)]
            across = (((0,), (0,)), ((), ()))
            acc8[m] = lax.dot_general(mine, rows, across, preferred_element_type=F32)
            dsend[slot, m] = lax.dot_general(theirs, rows, across, preferred_element_type=F32).astype(BF16)
            return 0

        lax.fori_loop(0, 8, combine, 0)

        @pl.when(k >= 2)
        def _():
            pl.semaphore_wait(free, 1)

        beside(k).start()

        wslot = weights_ready(5 * k + 4)

        def tile(j, _):
            c = cols(j, 256)
            acc8[0, :, c] += jnp.dot(hsv[...], wbuf[wslot, :, c], preferred_element_type=F32)
            return 0

        lax.fori_loop(0, DK // 256, tile, 0)

    def send_when_free(stage, k, p):
        @pl.when(k >= 2)
        def _():
            hop(stage, k, p).wait_send()

    def first(k):
        slot = lax.rem(k, 2)
        beside(k).wait_recv()
        for p, (row, size) in enumerate(PARTS):
            send_when_free(0, k, p)
            for pos in range(7, -1, -1):
                m = chip_at(turn(k, p), pos)
                v = acc8[m, row : row + size] + dland[slot, m, row : row + size].astype(F32)
                if pos >= 4:
                    a_send[p][slot, pos - 4] = v.astype(BF16)
                else:
                    acc4[slot, pos, row : row + size] = v
                if pos == 4:
                    hop(0, k, p).start()

        @pl.when(k + 2 < chunks)
        def _():
            pl.semaphore_signal(free, inc=1, device_id={"ep": at.partner}, device_id_type=MESH)

    def second(k):
        slot = lax.rem(k, 2)
        for p, (row, size) in enumerate(PARTS):
            hop(0, k, p).wait_recv()
            send_when_free(1, k, p)
            for pos in range(3, -1, -1):
                v = acc4[slot, pos, row : row + size] + a_land[p][k, pos].astype(F32)
                if pos >= 2:
                    b_send[p][slot, pos - 2] = v.astype(BF16)
                else:
                    acc2[slot, pos, row : row + size] = v
                if pos == 2:
                    hop(1, k, p).start()

    def third(k):
        slot = lax.rem(k, 2)
        for p, (row, size) in enumerate(PARTS):
            hop(1, k, p).wait_recv()
            send_when_free(2, k, p)
            for pos in (1, 0):
                v = acc2[slot, pos, row : row + size] + b_land[p][k, pos].astype(F32)
                if pos == 1:
                    c_send[p][slot, 0] = v.astype(BF16)
                    hop(2, k, p).start()
                else:
                    acc1[slot, row : row + size] = v

    def last(k):
        slot = lax.rem(k, 2)
        for p, (row, size) in enumerate(PARTS):
            hop(2, k, p).wait_recv()
            y[row : row + size, cols(k)] = (acc1[slot, row : row + size] + c_land[p][k, 0].astype(F32)).astype(BF16)

    def step(s, _):
        for stage, work in ((1, first), (0, compute), (2, second), (3, third), (4, last)):

            @pl.when(jnp.logical_and(s >= stage, s < chunks + stage))
            def _():
                work(s - stage)

        return 0

    lax.fori_loop(0, chunks + 4, step, 0)
    for k in (chunks - 2, chunks - 1):
        beside(k).wait_send()
        for stage in range(3):
            for p in range(3):
                hop(stage, k, p).wait_send()


def layer(x, expert, slot, gate, w_gate, w_up, w_down, s_gate, s_up, s_down):
    tokens, d_model = x.shape[2:]
    top = expert.shape[3]
    experts, _, ff = w_gate.shape
    slots = 5 * tokens * top // (4 * 64)
    chunks = d_model // DK
    rows = 16 * slots
    x = x.reshape(tokens, d_model)
    kept = jnp.where(slot < slots, expert * slots + slot, -1).astype(F32)
    route = jnp.concatenate([kept.reshape(tokens, top), gate.reshape(tokens, top)], axis=1).T

    dma, vmem, anyw = pltpu.SemaphoreType.DMA, pltpu.VMEM, pl.BlockSpec(memory_space=pl.ANY)
    here = pl.BlockSpec(memory_space=pltpu.VMEM)
    shape = jax.ShapeDtypeStruct
    landing = [shape((chunks, 8, size, DK), BF16) for _, size in PARTS]
    h, hs, g, *_ = pl.pallas_call(
        gather_kernel,
        name="gather_up",
        out_shape=[shape((experts, rows, ff), BF16), shape((tokens, ff), BF16), shape((8, 8 * slots, 2 * tokens), BF16)]
        + landing * 2,
        in_specs=[here, here] + [anyw] * 4,
        out_specs=[anyw] * 9,
        scratch_shapes=[
            vmem((16, 2 * top, tokens), F32),
            vmem((2, 8, 2 * tokens, DK), BF16),
            vmem((experts, rows, DK), BF16),
            vmem((3, DK, 2 * ff), BF16),
            vmem((experts, rows, 2 * ff), F32),
            vmem((tokens, 2 * ff), F32),
            vmem((8, 8 * slots, 2 * tokens), BF16),
            vmem((8 * slots, 2 * tokens), BF16),
            vmem((2, 64, ff), BF16),
            dma,
            dma((16,)),
            dma((3, chunks)),
            dma((5, 3)),
            dma((3, chunks)),
            dma((3, chunks)),
            dma((3, chunks)),
            dma((2, 3, chunks)),
            dma((2, 2)),
            dma((3,)),
            dma,
            dma((2,)),
        ],
        compiler_params=pltpu.CompilerParams(has_side_effects=True, vmem_limit_bytes=LIMIT),
    )(x, route, w_gate, w_up, s_gate, s_up)

    def by_part(lead, count):
        return [vmem((lead, count, size, DK), BF16) for _, size in PARTS]

    y = pl.pallas_call(
        scatter_kernel,
        name="down_scatter",
        out_shape=shape((tokens, d_model), BF16),
        in_specs=[anyw] * 5,
        out_specs=here,
        scratch_shapes=[
            vmem((experts, rows, ff), BF16),
            vmem((tokens, ff), BF16),
            vmem((8, 8 * slots, 2 * tokens), BF16),
            vmem((3, ff, DK), BF16),
            vmem((experts, rows, DK), BF16),
            vmem((2, 8, tokens, DK), BF16),
            vmem((2, 8, tokens, DK), BF16),
            vmem((8, tokens, DK), F32),
            vmem((2, 4, tokens, DK), F32),
            vmem((2, 2, tokens, DK), F32),
            vmem((2, tokens, DK), F32),
            *by_part(2, 4), *by_part(2, 2), *by_part(2, 1),
            *by_part(chunks, 4), *by_part(chunks, 2), *by_part(chunks, 1),
            dma((3,)),
            dma((3,)),
            dma((2,)),
            dma((2,)),
            pltpu.SemaphoreType.REGULAR,
            dma((3, 2)),
            dma((3, 2)),
            dma((3, 2)),
            dma((3, chunks)),
            dma((3, chunks)),
            dma((3, chunks)),
        ],
        compiler_params=pltpu.CompilerParams(has_side_effects=True, vmem_limit_bytes=LIMIT),
    )(h, hs, g, w_down, s_down)
    return y.reshape(1, 1, tokens, d_model)


def solution(mesh):
    by_device, by_expert = P("dp", "ep", None, None), P("ep", None, None)
    return jax.shard_map(
        layer,
        mesh=mesh,
        in_specs=(by_device,) * 4 + (by_expert,) * 3 + (P(None, None),) * 3,
        out_specs=by_device,
        check_vma=False,
    )
```

```python
import functools

import jax
import jax.numpy as jnp
from jax import lax
from jax.experimental import pallas as pl
from jax.experimental.pallas import tpu as pltpu
from jax.sharding import PartitionSpec as P

MESH = pl.DeviceIdType.MESH
DK = 512
PARTS = ((0, 96), (96, 80), (176, 80))
LIMIT = 67_000_000
F32, BF16 = jnp.float32, jnp.bfloat16


class Place:
    def __init__(self):
        self.me = lax.axis_index("ep")
        self.bits = [lax.rem(lax.div(self.me, m), 2) for m in (8, 4, 2)]
        self.core = lax.rem(self.me, 2)
        self.partner = self.me + 1 - 2 * self.core

    def across(self, d):
        ids = [self.me + m * (1 - 2 * b) for m, b in zip((8, 4, 2), self.bits)]
        return ids[0] * lax.div((1 - d) * (2 - d), 2) + ids[1] * (d * (2 - d)) + ids[2] * lax.div(d * (d - 1), 2)

    def chip(self, m):
        ms = (lax.div(m, 4), lax.rem(lax.div(m, 2), 2), lax.rem(m, 2))
        x, y, z = (b + s * (1 - 2 * b) for b, s in zip(self.bits, ms))
        return ((x * 2 + y) * 2 + z) * 2


def turn(o, i):
    return lax.rem(o + i, 3)


def chip_at(o, pos):
    m = 0
    for i in range(3):
        if pos >> i & 1:
            d = turn(o, i)
            m = m + 4 - 2 * d + lax.div(d * (d - 1), 2)
    return m


def cols(k, width=DK):
    return pl.ds(pl.multiple_of(k * width, width), width)


def gather_kernel(
    x, route, wg, wu, sg, su,
    h_out, hs_out, g_out, r0, r1, r2, q0, q1, q2,
    rt, xv, z, wbuf, acc, accs, sbuf, gbuf, hbuf,
    route_send, route_recv, fill, send, recv1, recv2, recv3, drecv, load, wsem, gsem, hsem,
):
    at = Place()
    me = at.me
    tokens, d_model = x.shape
    chunks = d_model // DK
    experts, slots = 4, 40
    ff = wg.shape[2]
    r, q = (r0, r1, r2), (q0, q1, q2)

    def remote(src, dst, s, v, dev):
        return pltpu.make_async_remote_copy(
            src_ref=src, dst_ref=dst, send_sem=s, recv_sem=v, device_id={"ep": dev}, device_id_type=MESH
        )

    def first(k, p):
        row, size = PARTS[p]
        return remote(x.at[pl.ds(row, size), cols(k)], r[p].at[k, 1], send.at[0, p], recv1.at[p, k], at.across(turn(k, p)))

    def second(k, p):
        return remote(
            r[p].at[k, pl.ds(0, 2)], r[p].at[k, pl.ds(2, 2)], send.at[1, p], recv2.at[p, k], at.across(turn(k, p + 1))
        )

    def third(k, p):
        return remote(
            r[p].at[k, pl.ds(0, 4)], r[p].at[k, pl.ds(4, 4)], send.at[2, p], recv3.at[p, k], at.across(turn(k, p + 2))
        )

    def beside(k, p, i):
        half = pl.ds(4 * i, 4)
        return remote(r[p].at[k, half], q[p].at[k, half], send.at[3 + i, p], drecv.at[i, p, k], at.partner)

    def filled(k, p):
        row, size = PARTS[p]
        return pltpu.make_async_copy(x.at[pl.ds(row, size), cols(k)], r[p].at[k, 0], fill.at[p, k])

    def weights(i):
        slot = lax.rem(i, 3)
        left, right = wbuf.at[slot, :, pl.ds(0, ff)], wbuf.at[slot, :, pl.ds(ff, ff)]

        @pl.when(i < chunks)
        def _():
            rows = cols(i)
            pltpu.make_async_copy(sg.at[rows], left, wsem.at[slot]).start()
            pltpu.make_async_copy(su.at[rows], right, wsem.at[slot]).start()

        @pl.when(jnp.logical_and(i >= chunks, i < 5 * chunks))
        def _():
            j = i - chunks
            e, rows = lax.rem(j, 4), cols(lax.div(j, 4))
            pltpu.make_async_copy(wg.at[e, rows], left, wsem.at[slot]).start()
            pltpu.make_async_copy(wu.at[e, rows], right, wsem.at[slot]).start()

    def weights_ready(i):
        slot = lax.rem(i, 3)
        pltpu.make_async_copy(wbuf.at[slot], wbuf.at[slot], wsem.at[slot]).wait()
        weights(i + 2)
        return slot

    def load_rows(k, src, core, i):
        slot = lax.rem(k, 2)
        for p, (row, size) in enumerate(PARTS):
            o = turn(k, p)
            for pos in range(8):
                dst = xv.at[slot, chip_at(o, pos), pl.ds(pl.multiple_of(core * tokens + row, 16), size)]
                pltpu.make_async_copy(src[p].at[k, pos], dst, load.at[slot, i]).start()

    def rows_ready(k, i):
        slot = lax.rem(k, 2)
        half = xv.at[slot, :, pl.ds(0, tokens)]
        pltpu.make_async_copy(half, half, load.at[slot, i]).wait()

    weights(0)
    weights(1)
    for j in range(1, 16):
        dev = lax.rem(me + j, 16)
        remote(route, rt.at[me], route_send, route_recv.at[me], dev).start()
    rt[me] = route[...]
    for p in range(3):
        first(0, p).start()
    for k in range(chunks):
        for p in range(3):
            filled(k, p).start()

    def build(m):
        base = at.chip(m)
        slot_of = lax.broadcasted_iota(jnp.int32, (80, tokens), 0)
        other = slot_of >= slots
        slot_of = jnp.where(other, slot_of - slots, slot_of)

        @pl.when(m >= 1)
        def _():
            pltpu.make_async_copy(gbuf, g_out.at[m - 1], gsem).wait()

        row = lax.broadcasted_iota(jnp.int32, (experts * slots, tokens), 0)
        for c in range(2):
            table = rt[base + c]
            want = (row + me * (experts * slots)).astype(F32)
            s = jnp.zeros((experts * slots, tokens), F32)
            for j in range(8):
                s = jnp.where(want == table[j : j + 1], 1.0, s)
            sbuf[m, c] = s.astype(BF16)

        def one(e, _):
            want = (slot_of + (me * experts + e) * slots).astype(F32)
            rows = pl.ds(pl.multiple_of(e * 80, 80), 80)
            for c in range(2):
                here = jnp.where(other == (c == 1), want, -2.0)
                table = rt[base + c]
                g = jnp.zeros((80, tokens), F32)
                for j in range(8):
                    g = jnp.where(here == table[j : j + 1], table[8 + j : 9 + j], g)
                gbuf[rows, c * tokens : (c + 1) * tokens] = g.astype(BF16)
            return 0

        lax.fori_loop(0, experts, one, 0)
        pltpu.make_async_copy(gbuf, g_out.at[m], gsem).start()

    def clear(e, _):
        acc[e] = jnp.zeros(acc.shape[1:], F32)
        return 0

    def shared(i):
        slot = weights_ready(i)
        accs[...] += jnp.dot(x[:, cols(i)], wbuf[slot], preferred_element_type=F32)

    def gathered(k):
        @pl.when(k < chunks)
        def _():
            for p in range(3):
                third(k, p).wait_recv()
                beside(k, p, 1).start()
            load_rows(k, r, at.core, 0)

    def exchanged(k):
        @pl.when(k < chunks)
        def _():
            for p in range(3):
                beside(k, p, 0).wait_recv()
                beside(k, p, 1).wait_recv()
            load_rows(k, q, 1 - at.core, 1)

    def compute(k):
        slot = lax.rem(k, 2)

        for m in range(8):
            d = [
                jnp.dot(sbuf[m, c], xv[slot, m, c * tokens : (c + 1) * tokens], preferred_element_type=F32)
                for c in range(2)
            ]
            for e in range(experts):
                mine = [v[e * slots : (e + 1) * slots] for v in d]
                z[e, m * 80 : (m + 1) * 80] = jnp.concatenate(mine, axis=0).astype(BF16)

        def expert(e, _):
            pl.when(e == 1)(lambda: gathered(k + 1))
            pl.when(e == 3)(lambda: exchanged(k + 1))
            wslot = weights_ready(chunks + 4 * k + e)

            acc[e] += jnp.dot(z[e], wbuf[wslot], preferred_element_type=F32)
            return 0

        lax.fori_loop(0, experts, expert, 0)

    def step(s, _):
        @pl.when(s + 1 < chunks)
        def _():
            for p in range(3):
                first(s + 1, p).start()

        @pl.when(jnp.logical_and(s >= 1, s < chunks + 1))
        def _():
            k = s - 1
            for p in range(3):
                filled(k, p).wait()
                first(k, p).wait_recv()
                second(k, p).start()

        @pl.when(jnp.logical_and(s >= 2, s < chunks + 2))
        def _():
            k = s - 2
            for p in range(3):
                second(k, p).wait_recv()
                third(k, p).start()
                beside(k, p, 0).start()

        @pl.when(s == 0)
        def _():
            accs[...] = jnp.zeros(accs.shape, F32)

        @pl.when(s < 4)
        def _():
            clear(s, 0)
            shared(2 * s)
            shared(2 * s + 1)

        @pl.when(s == 2)
        def _():
            for j in range(1, 16):
                b = lax.rem(me + j, 16)
                remote(route, rt.at[b], route_send, route_recv.at[b], b).wait_recv()

            def one(m, _):
                build(m)
                return 0

            lax.fori_loop(0, 8, one, 0)
            pltpu.make_async_copy(gbuf, g_out.at[7], gsem).wait()

        @pl.when(s == 3)
        def _():
            gathered(0)
            exchanged(0)

        @pl.when(s >= 4)
        def _():
            k = s - 4
            rows_ready(k, 0)
            rows_ready(k, 1)
            compute(k)

        return 0

    lax.fori_loop(0, chunks + 4, step, 0)

    def hidden(src, dst, i, rows):
        slot = lax.rem(i, 2)

        @pl.when(i >= 2)
        def _():
            pltpu.make_async_copy(hbuf.at[slot], dst, hsem.at[slot]).wait()

        a = src[rows, pl.ds(0, ff)]
        hbuf[slot] = (a * jax.nn.sigmoid(a) * src[rows, pl.ds(ff, ff)]).astype(BF16)
        pltpu.make_async_copy(hbuf.at[slot], dst, hsem.at[slot]).start()

    def routed(i, _):
        e, rows = lax.div(i, 10), pl.ds(pl.multiple_of(lax.rem(i, 10) * 64, 64), 64)
        hidden(acc.at[e], h_out.at[e, rows], i, rows)
        return 0

    lax.fori_loop(0, 10 * experts, routed, 0)

    def common(i, _):
        rows = pl.ds(pl.multiple_of(i * 64, 64), 64)
        hidden(accs, hs_out.at[rows], i + 10 * experts, rows)
        return 0

    lax.fori_loop(0, tokens // 64, common, 0)
    for slot in range(2):
        pltpu.make_async_copy(hbuf.at[slot], hs_out.at[pl.ds(0, 64)], hsem.at[slot]).wait()

    remote(rt.at[pl.ds(0, 15)], rt.at[pl.ds(0, 15)], route_send, route_recv.at[0], at.partner).wait_send()
    for p in range(3):
        one, two, four, rest = r[p].at[:, 0], r[p].at[:, pl.ds(0, 2)], r[p].at[:, pl.ds(0, 4)], r[p].at[:, pl.ds(4, 4)]
        for i, sent in enumerate((one, two, four, four, rest)):
            remote(sent, sent, send.at[i, p], recv1.at[p, 0], at.partner).wait_send()


def scatter_kernel(
    h, hs, g, wd, sd,
    y,
    hv, hsv, gv, wbuf, o, dsend, dland, acc8, acc4, acc2, acc1,
    as0, as1, as2, bs0, bs1, bs2, cs0, cs1, cs2,
    al0, al1, al2, bl0, bl1, bl2, cl0, cl1, cl2,
    start_sem, wsem, dsend_sem, drecv, free, asend_sem, bsend_sem, csend_sem, arecv, brecv, crecv,
):
    at = Place()
    tokens, d_model = y.shape
    chunks = d_model // DK
    experts = h.shape[0]
    ff = h.shape[2]
    a_send, b_send, c_send = (as0, as1, as2), (bs0, bs1, bs2), (cs0, cs1, cs2)
    a_land, b_land, c_land = (al0, al1, al2), (bl0, bl1, bl2), (cl0, cl1, cl2)

    def remote(src, dst, s, v, dev):
        return pltpu.make_async_remote_copy(
            src_ref=src, dst_ref=dst, send_sem=s, recv_sem=v, device_id={"ep": dev}, device_id_type=MESH
        )

    def beside(k):
        slot = lax.rem(k, 2)
        return remote(dsend.at[slot], dland.at[slot], dsend_sem.at[slot], drecv.at[slot], at.partner)

    def hop(stage, k, p):
        slot = lax.rem(k, 2)
        src, dst = (a_send, b_send, c_send)[stage][p], (a_land, b_land, c_land)[stage][p]
        sems, lands = (asend_sem, bsend_sem, csend_sem)[stage], (arecv, brecv, crecv)[stage]
        return remote(src.at[slot], dst.at[k], sems.at[p, slot], lands.at[p, k], at.across(turn(k, p + 2 - stage)))

    def weights(i):
        slot = lax.rem(i, 3)
        k, e = lax.div(i, 5), lax.rem(i, 5)

        @pl.when(jnp.logical_and(i < 5 * chunks, e < 4))
        def _():
            pltpu.make_async_copy(wd.at[e, :, cols(k)], wbuf.at[slot], wsem.at[slot]).start()

        @pl.when(jnp.logical_and(i < 5 * chunks, e == 4))
        def _():
            pltpu.make_async_copy(sd.at[:, cols(k)], wbuf.at[slot], wsem.at[slot]).start()

    def weights_ready(i):
        slot = lax.rem(i, 3)
        pltpu.make_async_copy(wbuf.at[slot], wbuf.at[slot], wsem.at[slot]).wait()
        weights(i + 2)
        return slot

    def hidden(e):
        return pltpu.make_async_copy(h.at[e], hv.at[e], start_sem.at[e])

    common = pltpu.make_async_copy(hs, hsv, start_sem.at[4])
    gates = pltpu.make_async_copy(g, gv, start_sem.at[5])
    hidden(0).start()
    weights(0)
    hidden(1).start()
    weights(1)
    for copy in (hidden(2), hidden(3), gates, common):
        copy.start()

    def compute(k):
        slot = lax.rem(k, 2)

        def expert(e, _):
            pl.when(k == 0)(lambda: hidden(e).wait())
            wslot = weights_ready(5 * k + e)
            o[e] = jnp.dot(hv[e], wbuf[wslot], preferred_element_type=F32).astype(BF16)
            return 0

        lax.fori_loop(0, experts, expert, 0)

        @pl.when(k == 0)
        def _():
            gates.wait()
            common.wait()

        @pl.when(k >= 2)
        def _():
            beside(k).wait_send()

        def combine(m, core):
            rows = o[:, m * 80 : (m + 1) * 80, :].reshape(4 * 80, DK)
            return lax.dot_general(gv[m, :, cols(core, 256)], rows, (((0,), (0,)), ((), ())), preferred_element_type=F32)

        for m in range(8):
            dsend[slot, m] = combine(m, 1 - at.core).astype(BF16)

        @pl.when(k >= 2)
        def _():
            pl.semaphore_wait(free, 1)

        beside(k).start()
        for m in range(8):
            acc8[m] = combine(m, at.core)
        wslot = weights_ready(5 * k + 4)
        acc8[0] += jnp.dot(hsv[...], wbuf[wslot], preferred_element_type=F32)

    def send_when_free(stage, k, p):
        @pl.when(k >= 2)
        def _():
            hop(stage, k, p).wait_send()

    def first(k):
        slot = lax.rem(k, 2)
        beside(k).wait_recv()
        for p, (row, size) in enumerate(PARTS):
            send_when_free(0, k, p)
            for pos in range(7, -1, -1):
                m = chip_at(turn(k, p), pos)
                v = acc8[m, row : row + size] + dland[slot, m, row : row + size].astype(F32)
                if pos >= 4:
                    a_send[p][slot, pos - 4] = v.astype(BF16)
                else:
                    acc4[slot, pos, row : row + size] = v
                if pos == 4:
                    hop(0, k, p).start()

        @pl.when(k + 2 < chunks)
        def _():
            pl.semaphore_signal(free, inc=1, device_id={"ep": at.partner}, device_id_type=MESH)

    def second(k):
        slot = lax.rem(k, 2)
        for p, (row, size) in enumerate(PARTS):
            hop(0, k, p).wait_recv()
            send_when_free(1, k, p)
            for pos in range(3, -1, -1):
                v = acc4[slot, pos, row : row + size] + a_land[p][k, pos].astype(F32)
                if pos >= 2:
                    b_send[p][slot, pos - 2] = v.astype(BF16)
                else:
                    acc2[slot, pos, row : row + size] = v
                if pos == 2:
                    hop(1, k, p).start()

    def third(k):
        slot = lax.rem(k, 2)
        for p, (row, size) in enumerate(PARTS):
            hop(1, k, p).wait_recv()
            send_when_free(2, k, p)
            for pos in (1, 0):
                v = acc2[slot, pos, row : row + size] + b_land[p][k, pos].astype(F32)
                if pos == 1:
                    c_send[p][slot, 0] = v.astype(BF16)
                    hop(2, k, p).start()
                else:
                    acc1[slot, row : row + size] = v

    def last(k):
        slot = lax.rem(k, 2)
        for p, (row, size) in enumerate(PARTS):
            hop(2, k, p).wait_recv()
            y[row : row + size, cols(k)] = (acc1[slot, row : row + size] + c_land[p][k, 0].astype(F32)).astype(BF16)

    def step(s, _):
        for stage, work in ((1, first), (0, compute), (2, second), (3, third), (4, last)):

            @pl.when(jnp.logical_and(s >= stage, s < chunks + stage))
            def _():
                work(s - stage)

        return 0

    lax.fori_loop(0, chunks + 4, step, 0)
    for k in (chunks - 2, chunks - 1):
        beside(k).wait_send()
        for stage in range(3):
            for p in range(3):
                hop(stage, k, p).wait_send()


def layer(x, expert, slot, gate, w_gate, w_up, w_down, s_gate, s_up, s_down):
    tokens, d_model = x.shape[2:]
    top = expert.shape[3]
    experts, _, ff = w_gate.shape
    slots = 5 * tokens * top // (4 * 64)
    chunks = d_model // DK
    rows = 16 * slots
    x = x.reshape(tokens, d_model)
    kept = jnp.where(slot < slots, expert * slots + slot, -1).astype(F32)
    route = jnp.concatenate([kept.reshape(tokens, top), gate.reshape(tokens, top)], axis=1).T

    dma, vmem, anyw = pltpu.SemaphoreType.DMA, pltpu.VMEM, pl.BlockSpec(memory_space=pl.ANY)
    here = pl.BlockSpec(memory_space=pltpu.VMEM)
    shape = jax.ShapeDtypeStruct
    landing = [shape((chunks, 8, size, DK), BF16) for _, size in PARTS]
    h, hs, g, *_ = pl.pallas_call(
        gather_kernel,
        name="gather_up",
        out_shape=[shape((experts, rows, ff), BF16), shape((tokens, ff), BF16), shape((8, 8 * slots, 2 * tokens), BF16)]
        + landing * 2,
        in_specs=[here, here] + [anyw] * 4,
        out_specs=[anyw] * 9,
        scratch_shapes=[
            vmem((16, 2 * top, tokens), F32),
            vmem((2, 8, 2 * tokens, DK), BF16),
            vmem((experts, rows, DK), BF16),
            vmem((3, DK, 2 * ff), BF16),
            vmem((experts, rows, 2 * ff), F32),
            vmem((tokens, 2 * ff), F32),
            vmem((8, 2, experts * slots, tokens), BF16),
            vmem((8 * slots, 2 * tokens), BF16),
            vmem((2, 64, ff), BF16),
            dma,
            dma((16,)),
            dma((3, chunks)),
            dma((5, 3)),
            dma((3, chunks)),
            dma((3, chunks)),
            dma((3, chunks)),
            dma((2, 3, chunks)),
            dma((2, 2)),
            dma((3,)),
            dma,
            dma((2,)),
        ],
        compiler_params=pltpu.CompilerParams(has_side_effects=True, vmem_limit_bytes=LIMIT),
    )(x, route, w_gate, w_up, s_gate, s_up)

    def by_part(lead, count):
        return [vmem((lead, count, size, DK), BF16) for _, size in PARTS]

    y = pl.pallas_call(
        scatter_kernel,
        name="down_scatter",
        out_shape=shape((tokens, d_model), BF16),
        in_specs=[anyw] * 5,
        out_specs=here,
        scratch_shapes=[
            vmem((experts, rows, ff), BF16),
            vmem((tokens, ff), BF16),
            vmem((8, 8 * slots, 2 * tokens), BF16),
            vmem((3, ff, DK), BF16),
            vmem((experts, rows, DK), BF16),
            vmem((2, 8, tokens, DK), BF16),
            vmem((2, 8, tokens, DK), BF16),
            vmem((8, tokens, DK), F32),
            vmem((2, 4, tokens, DK), F32),
            vmem((2, 2, tokens, DK), F32),
            vmem((2, tokens, DK), F32),
            *by_part(2, 4), *by_part(2, 2), *by_part(2, 1),
            *by_part(chunks, 4), *by_part(chunks, 2), *by_part(chunks, 1),
            dma((6,)),
            dma((3,)),
            dma((2,)),
            dma((2,)),
            pltpu.SemaphoreType.REGULAR,
            dma((3, 2)),
            dma((3, 2)),
            dma((3, 2)),
            dma((3, chunks)),
            dma((3, chunks)),
            dma((3, chunks)),
        ],
        compiler_params=pltpu.CompilerParams(has_side_effects=True, vmem_limit_bytes=LIMIT),
    )(h, hs, g, w_down, s_down)
    return y.reshape(1, 1, tokens, d_model)


def solution(mesh):
    by_device, by_expert = P("dp", "ep", None, None), P("ep", None, None)
    return jax.shard_map(
        layer,
        mesh=mesh,
        in_specs=(by_device,) * 4 + (by_expert,) * 3 + (P(None, None),) * 3,
        out_specs=by_device,
        check_vma=False,
    )
```

```python
import functools

import jax
import jax.numpy as jnp
from jax import lax
from jax.experimental import pallas as pl
from jax.experimental.pallas import tpu as pltpu
from jax.sharding import PartitionSpec as P

MESH = pl.DeviceIdType.MESH
DK = 512
DN = 256
PARTS = ((0, 96), (96, 80), (176, 80))
LIMIT = 67_000_000
TAIL_UP, TAIL_DOWN = 3, 1
AHEAD = 2
F32, BF16 = jnp.float32, jnp.bfloat16


class Place:
    def __init__(self):
        self.me = lax.axis_index("ep")
        self.bits = [lax.rem(lax.div(self.me, m), 2) for m in (8, 4, 2)]
        self.core = lax.rem(self.me, 2)
        self.partner = self.me + 1 - 2 * self.core

    def across(self, d):
        ids = [self.me + m * (1 - 2 * b) for m, b in zip((8, 4, 2), self.bits)]
        return ids[0] * lax.div((1 - d) * (2 - d), 2) + ids[1] * (d * (2 - d)) + ids[2] * lax.div(d * (d - 1), 2)

    def chip(self, m):
        ms = (lax.div(m, 4), lax.rem(lax.div(m, 2), 2), lax.rem(m, 2))
        x, y, z = (b + s * (1 - 2 * b) for b, s in zip(self.bits, ms))
        return ((x * 2 + y) * 2 + z) * 2


def turn(o, i):
    return lax.rem(o + i, 3)


def chip_at(o, pos):
    m = 0
    for i in range(3):
        if pos >> i & 1:
            d = turn(o, i)
            m = m + 4 - 2 * d + lax.div(d * (d - 1), 2)
    return m


def cols(k, width):
    return pl.ds(pl.multiple_of(k * width, width), width)


class Chunks:
    def __init__(self, d_model, tail):
        self.count = 1 + (d_model - (1 + tail) * DN) // DK + tail
        self.tail = self.count - tail

    def width(self, k):
        return DK if 0 < k < self.tail else DN

    def of(self, k, width):
        if isinstance(k, int):
            start = sum(self.width(i) for i in range(k))
        else:
            started = lax.div(k + self.count - 1, self.count)
            late = (k - self.tail) * lax.div(k, self.tail + 1)
            start = k * DK - (DK - DN) * (started + late)
        return pl.ds(pl.multiple_of(start, DN), width)

    def when(self, cond, k, work):
        narrow = jnp.logical_or(k == 0, jnp.logical_and(k >= self.tail, k < self.count))
        wide = jnp.logical_and(k > 0, k < self.tail)
        pl.when(jnp.logical_and(cond, narrow))(lambda: work(k, DN))
        pl.when(jnp.logical_and(cond, wide))(lambda: work(k, DK))


def gather_kernel(
    x, route, wg, wu, sg, su,
    h_out, hs_out, g_out, r0, r1, r2, q0, q1, q2,
    rt, xv, z, wbuf, acc, accs, sbuf, gbuf, hbuf,
    route_send, route_recv, fill, send, recv1, recv2, recv3, drecv, load, wsem, gsem, hsem,
):
    at = Place()
    me = at.me
    tokens, d_model = x.shape
    part = Chunks(d_model, TAIL_UP)
    chunks = part.count
    experts, slots = 4, 40
    ff = wg.shape[2]
    r, q = (r0, r1, r2), (q0, q1, q2)

    def remote(src, dst, s, v, dev):
        return pltpu.make_async_remote_copy(
            src_ref=src, dst_ref=dst, send_sem=s, recv_sem=v, device_id={"ep": dev}, device_id_type=MESH
        )

    def first(k, w, p):
        row, size = PARTS[p]
        src, dst = x.at[pl.ds(row, size), part.of(k, w)], r[p].at[k, 1, :, pl.ds(0, w)]
        return remote(src, dst, send.at[0, p], recv1.at[p, k], at.across(turn(k, p)))

    def onward(k, w, p, i):
        n = 2 << i
        src, dst = r[p].at[k, pl.ds(0, n), :, pl.ds(0, w)], r[p].at[k, pl.ds(n, n), :, pl.ds(0, w)]
        return remote(src, dst, send.at[1 + i, p], (recv2, recv3)[i].at[p, k], at.across(turn(k, p + 1 + i)))

    def beside(k, w, p, i):
        half = pl.ds(4 * i, 4)
        src, dst = r[p].at[k, half, :, pl.ds(0, w)], q[p].at[k, half, :, pl.ds(0, w)]
        return remote(src, dst, send.at[3 + i, p], drecv.at[i, p, k], at.partner)

    def filled(k, w, p):
        row, size = PARTS[p]
        return pltpu.make_async_copy(
            x.at[pl.ds(row, size), part.of(k, w)], r[p].at[k, 0, :, pl.ds(0, w)], fill.at[p, k]
        )

    def weights(i):
        slot = lax.rem(i, 3)

        def fetch(gate, up, k, w):
            rows = part.of(k, w)
            for ref, start in ((gate, 0), (up, ff)):
                dst = wbuf.at[slot, pl.ds(0, w), pl.ds(start, ff)]
                pltpu.make_async_copy(ref.at[rows], dst, wsem.at[slot]).start()

        def common(k):
            part.when(True, k, lambda k, w: fetch(sg, su, k, w))

        def routed(e, k):
            part.when(True, k, lambda k, w: fetch(wg.at[e], wu.at[e], k, w))

        rest = i - chunks
        pl.when(rest < 0)(lambda: common(i))
        pl.when(rest >= 0)(lambda: routed(lax.rem(rest, 4), lax.div(rest, 4)))

    def weights_ready(i, w):
        slot = lax.rem(i, 3)
        rows = wbuf.at[slot, pl.ds(0, w)]
        pltpu.make_async_copy(rows, rows, wsem.at[slot]).wait()
        weights(i + 2)
        return slot

    def load_rows(k, w, src, core, i):
        slot = lax.rem(k, 2)
        for p, (row, size) in enumerate(PARTS):
            o = turn(k, p)
            for pos in range(8):
                rows = pl.ds(pl.multiple_of(core * tokens + row, 16), size)
                dst = xv.at[slot, chip_at(o, pos), rows, pl.ds(0, w)]
                pltpu.make_async_copy(src[p].at[k, pos, :, pl.ds(0, w)], dst, load.at[slot, i]).start()

    def rows_ready(k, w, i):
        slot = lax.rem(k, 2)
        half = xv.at[slot, :, pl.ds(0, tokens), pl.ds(0, w)]
        pltpu.make_async_copy(half, half, load.at[slot, i]).wait()

    def begin(k, w):
        for p in range(3):
            first(k, w, p).start()

    for k in range(AHEAD):
        begin(k, part.width(k))
    weights(0)
    weights(1)
    for k in range(chunks):
        for p in range(3):
            filled(k, part.width(k), p).start()
    for j in range(1, 16):
        dev = lax.rem(me + j, 16)
        remote(route, rt.at[me], route_send, route_recv.at[me], dev).start()
    rt[me] = route[...]

    def build(m):
        base = at.chip(m)
        row = lax.broadcasted_iota(jnp.int32, (slots, tokens), 0)
        none = jnp.zeros((slots, tokens), F32)

        slot = lax.rem(m, 2)

        @pl.when(m >= 2)
        def _():
            pltpu.make_async_copy(gbuf.at[slot], g_out.at[m - 2], gsem.at[slot]).wait()

        for c in range(2):
            table = rt[base + c]
            hits = []
            for e in range(experts):
                want = (row + (me * experts + e) * slots).astype(F32)
                s, g = none, none
                for j in range(8):
                    hit = want == table[j : j + 1]
                    s = jnp.where(hit, 1.0, s)
                    g = jnp.where(hit, table[8 + j : 9 + j], g)
                hits.append(s)
                both = jnp.concatenate([g, none] if c == 0 else [none, g], axis=0)
                gbuf[slot, e * 80 : (e + 1) * 80, c * tokens : (c + 1) * tokens] = both.astype(BF16)
            sbuf[m, c] = jnp.concatenate(hits, axis=0).astype(BF16)
        pltpu.make_async_copy(gbuf.at[slot], g_out.at[m], gsem.at[slot]).start()

    def accumulate(ref, k, w, a, b):
        if w == DN:

            @pl.when(k == 0)
            def _():
                ref[...] = jnp.dot(a[...], b[...], preferred_element_type=F32)

            @pl.when(k > 0)
            def _():
                ref[...] += jnp.dot(a[...], b[...], preferred_element_type=F32)
        else:
            ref[...] += jnp.dot(a[...], b[...], preferred_element_type=F32)

    def shared(i, w):
        slot = weights_ready(i, w)
        accumulate(accs, i, w, x.at[:, part.of(i, w)], wbuf.at[slot, pl.ds(0, w)])

    def hidden(src, dst, i, rows):
        slot = lax.rem(i, 8)

        @pl.when(i >= 8)
        def _():
            pltpu.make_async_copy(hbuf.at[slot], dst, hsem.at[slot]).wait()

        a = src[rows, pl.ds(0, ff)]
        hbuf[slot] = (a * jax.nn.sigmoid(a) * src[rows, pl.ds(ff, ff)]).astype(BF16)
        pltpu.make_async_copy(hbuf.at[slot], dst, hsem.at[slot]).start()

    def hidden_shared():
        def one(i, _):
            rows = pl.ds(pl.multiple_of(i * 64, 64), 64)
            hidden(accs, hs_out.at[rows], i, rows)
            return 0

        lax.fori_loop(0, tokens // 64, one, 0)

    def hidden_routed(e):
        def one(i, _):
            rows = pl.ds(pl.multiple_of(i * 64, 64), 64)
            hidden(acc.at[e], h_out.at[e, rows], tokens // 64 + 10 * e + i, rows)
            return 0

        lax.fori_loop(0, 10, one, 0)

    def gathered(k, w):
        for p in range(3):
            onward(k, w, p, 1).wait_recv()
            beside(k, w, p, 1).start()
        load_rows(k, w, r, at.core, 0)

    def exchanged(k, w):
        for p in range(3):
            beside(k, w, p, 0).wait_recv()
            beside(k, w, p, 1).wait_recv()
        load_rows(k, w, q, 1 - at.core, 1)

    def compute(k, w):
        slot = lax.rem(k, 2)
        rows_ready(k, w, 0)
        rows_ready(k, w, 1)
        for m in range(8):
            d = [
                jnp.dot(sbuf[m, c], xv[slot, m, c * tokens : (c + 1) * tokens, :w], preferred_element_type=F32)
                for c in range(2)
            ]
            for e in range(experts):
                mine = [v[e * slots : (e + 1) * slots] for v in d]
                z[e, m * 80 : (m + 1) * 80, :w] = jnp.concatenate(mine, axis=0).astype(BF16)

        def expert(e, _):
            part.when(e == 1, k + 2, third)
            part.when(e == 2, k + 1, gathered)
            part.when(e == 3, k + 1, exchanged)
            wslot = weights_ready(chunks + 4 * k + e, w)
            accumulate(acc.at[e], k, w, z.at[e, :, pl.ds(0, w)], wbuf.at[wslot, pl.ds(0, w)])
            if w == DN:
                pl.when(k == chunks - 1)(lambda: hidden_routed(e))
            return 0

        lax.fori_loop(0, experts, expert, 0)

    def second(k, w):
        for p in range(3):
            filled(k, w, p).wait()
            first(k, w, p).wait_recv()
            onward(k, w, p, 0).start()

    def third(k, w):
        for p in range(3):
            onward(k, w, p, 0).wait_recv()
            onward(k, w, p, 1).start()
            beside(k, w, p, 0).start()

    def tables():
        for j in range(1, 16):
            b = lax.rem(me + j, 16)
            remote(route, rt.at[b], route_send, route_recv.at[b], b).wait_recv()

        def one(m, _):
            build(m)
            return 0

        lax.fori_loop(0, 8, one, 0)
        for slot in range(2):
            pltpu.make_async_copy(gbuf.at[slot], g_out.at[slot], gsem.at[slot]).wait()

    def shared_between(lo, hi):
        def one(i, _):
            part.when(True, i, shared)
            return 0

        lax.fori_loop(lo, hi, one, 0)

    def step(s, _):
        pl.when(s == 0)(lambda: shared_between(0, 3))
        part.when(s == 2, s - 1, third)
        part.when(True, s, second)
        part.when(True, s + AHEAD, begin)
        pl.when(s == 1)(lambda: shared_between(3, 6))
        part.when(s == 1, s - 1, third)
        pl.when(s == 1)(tables)
        pl.when(s == 2)(lambda: shared_between(6, chunks))
        part.when(s == 2, s - 2, gathered)
        part.when(s == 2, s - 2, exchanged)
        part.when(True, s - 3, compute)
        pl.when(s == 3)(hidden_shared)
        return 0

    lax.fori_loop(0, chunks + 3, step, 0)

    for slot in range(8):
        pltpu.make_async_copy(hbuf.at[slot], hs_out.at[pl.ds(0, 64)], hsem.at[slot]).wait()

    remote(rt.at[pl.ds(0, 15)], rt.at[pl.ds(0, 15)], route_send, route_recv.at[0], at.partner).wait_send()
    for p in range(3):
        for i, rows in enumerate((pl.ds(0, 1), pl.ds(0, 2), pl.ds(0, 4), pl.ds(0, 4), pl.ds(4, 4))):
            sent = r[p].at[pl.ds(0, d_model // DK), rows]
            remote(sent, sent, send.at[i, p], recv1.at[p, 0], at.partner).wait_send()


def scatter_kernel(
    h, hs, g, wd, sd,
    y,
    hv, hsv, gv, wbuf, o, dsend, dland, acc8, acc4, acc2, acc1,
    as0, as1, as2, bs0, bs1, bs2, cs0, cs1, cs2,
    al0, al1, al2, bl0, bl1, bl2, cl0, cl1, cl2,
    start_sem, wsem, dsend_sem, drecv, free, asend_sem, bsend_sem, csend_sem, arecv, brecv, crecv,
):
    at = Place()
    tokens, d_model = y.shape
    part = Chunks(d_model, TAIL_DOWN)
    chunks = part.count
    experts = h.shape[0]
    ff = h.shape[2]
    a_send, b_send, c_send = (as0, as1, as2), (bs0, bs1, bs2), (cs0, cs1, cs2)
    a_land, b_land, c_land = (al0, al1, al2), (bl0, bl1, bl2), (cl0, cl1, cl2)

    def remote(src, dst, s, v, dev):
        return pltpu.make_async_remote_copy(
            src_ref=src, dst_ref=dst, send_sem=s, recv_sem=v, device_id={"ep": dev}, device_id_type=MESH
        )

    def beside(k, w):
        slot = lax.rem(k, 2)
        src, dst = dsend.at[slot, :, :, pl.ds(0, w)], dland.at[slot, :, :, pl.ds(0, w)]
        return remote(src, dst, dsend_sem.at[slot], drecv.at[slot], at.partner)

    def hop(stage, k, w, p):
        slot = lax.rem(k, 2)
        src, dst = (a_send, b_send, c_send)[stage][p], (a_land, b_land, c_land)[stage][p]
        sems, lands = (asend_sem, bsend_sem, csend_sem)[stage], (arecv, brecv, crecv)[stage]
        src, dst = src.at[slot, :, :, pl.ds(0, w)], dst.at[k, :, :, pl.ds(0, w)]
        return remote(src, dst, sems.at[p, slot], lands.at[p, k], at.across(turn(k, p + 2 - stage)))

    def weights(i):
        slot = lax.rem(i, 3)
        e = lax.rem(i, 5)

        def fetch(k, w):
            dst = wbuf.at[slot, :, pl.ds(0, w)]
            pl.when(e < 4)(lambda: pltpu.make_async_copy(wd.at[e, :, part.of(k, w)], dst, wsem.at[slot]).start())
            pl.when(e == 4)(lambda: pltpu.make_async_copy(sd.at[:, part.of(k, w)], dst, wsem.at[slot]).start())

        part.when(True, lax.div(i, 5), fetch)

    def weights_ready(i, w):
        slot = lax.rem(i, 3)
        columns = wbuf.at[slot, :, pl.ds(0, w)]
        pltpu.make_async_copy(columns, columns, wsem.at[slot]).wait()
        weights(i + 2)
        return slot

    def hidden(e):
        return pltpu.make_async_copy(h.at[e], hv.at[e], start_sem.at[e])

    common = pltpu.make_async_copy(hs, hsv, start_sem.at[4])
    gates = pltpu.make_async_copy(g, gv, start_sem.at[5])
    hidden(0).start()
    weights(0)
    hidden(1).start()
    weights(1)
    for copy in (hidden(2), hidden(3), gates, common):
        copy.start()

    def compute(k, w):
        slot = lax.rem(k, 2)

        def expert(e, _):
            pl.when(k == 0)(lambda: hidden(e).wait())
            wslot = weights_ready(5 * k + e, w)
            o[e, :, :w] = jnp.dot(hv[e], wbuf[wslot, :, :w], preferred_element_type=F32).astype(BF16)
            return 0

        lax.fori_loop(0, experts, expert, 0)

        @pl.when(k == 0)
        def _():
            gates.wait()
            common.wait()

        sent(k, lambda v: beside(k, v).wait_send())

        def combine(m, core):
            rows = o[:, m * 80 : (m + 1) * 80, :w].reshape(4 * 80, w)
            return lax.dot_general(gv[m, :, cols(core, 256)], rows, (((0,), (0,)), ((), ())), preferred_element_type=F32)

        for m in range(8):
            dsend[slot, m, :, :w] = combine(m, 1 - at.core).astype(BF16)

        @pl.when(k >= 2)
        def _():
            pl.semaphore_wait(free, 1)

        beside(k, w).start()
        for m in range(8):
            acc8[m, :, :w] = combine(m, at.core)
        wslot = weights_ready(5 * k + 4, w)
        acc8[0, :, :w] += jnp.dot(hsv[...], wbuf[wslot, :, :w], preferred_element_type=F32)

    def sent(k, wait):
        narrow = jnp.logical_or(k == 2, k - 2 >= part.tail)
        pl.when(narrow)(lambda: wait(DN))
        pl.when(jnp.logical_and(k > 2, k - 2 < part.tail))(lambda: wait(DK))

    def first(k, w):
        slot = lax.rem(k, 2)
        beside(k, w).wait_recv()
        for p, (row, size) in enumerate(PARTS):
            sent(k, lambda v: hop(0, k, v, p).wait_send())
            for pos in range(7, -1, -1):
                m = chip_at(turn(k, p), pos)
                v = acc8[m, row : row + size, :w] + dland[slot, m, row : row + size, :w].astype(F32)
                if pos >= 4:
                    a_send[p][slot, pos - 4, :, :w] = v.astype(BF16)
                else:
                    acc4[slot, pos, row : row + size, :w] = v
                if pos == 4:
                    hop(0, k, w, p).start()

        @pl.when(k + 2 < chunks)
        def _():
            pl.semaphore_signal(free, inc=1, device_id={"ep": at.partner}, device_id_type=MESH)

    def second(k, w):
        slot = lax.rem(k, 2)
        for p, (row, size) in enumerate(PARTS):
            hop(0, k, w, p).wait_recv()
            sent(k, lambda v: hop(1, k, v, p).wait_send())
            for pos in range(3, -1, -1):
                v = acc4[slot, pos, row : row + size, :w] + a_land[p][k, pos, :, :w].astype(F32)
                if pos >= 2:
                    b_send[p][slot, pos - 2, :, :w] = v.astype(BF16)
                else:
                    acc2[slot, pos, row : row + size, :w] = v
                if pos == 2:
                    hop(1, k, w, p).start()

    def third(k, w):
        slot = lax.rem(k, 2)
        for p, (row, size) in enumerate(PARTS):
            hop(1, k, w, p).wait_recv()
            sent(k, lambda v: hop(2, k, v, p).wait_send())
            for pos in (1, 0):
                v = acc2[slot, pos, row : row + size, :w] + b_land[p][k, pos, :, :w].astype(F32)
                if pos == 1:
                    c_send[p][slot, 0, :, :w] = v.astype(BF16)
                    hop(2, k, w, p).start()
                else:
                    acc1[slot, row : row + size, :w] = v

    def last(k, w):
        slot = lax.rem(k, 2)
        for p, (row, size) in enumerate(PARTS):
            hop(2, k, w, p).wait_recv()
            out = acc1[slot, row : row + size, :w] + c_land[p][k, 0, :, :w].astype(F32)
            y[row : row + size, part.of(k, w)] = out.astype(BF16)

    def step(s, _):
        for stage, work in ((1, first), (0, compute), (2, second), (3, third), (4, last)):
            part.when(True, s - stage, work)
        return 0

    lax.fori_loop(0, chunks + 4, step, 0)
    for k, w in ((chunks - 2, part.width(chunks - 2)), (chunks - 1, DN)):
        beside(k, w).wait_send()
        for stage in range(3):
            for p in range(3):
                hop(stage, k, w, p).wait_send()


def layer(x, expert, slot, gate, w_gate, w_up, w_down, s_gate, s_up, s_down):
    tokens, d_model = x.shape[2:]
    top = expert.shape[3]
    experts, _, ff = w_gate.shape
    slots = 5 * tokens * top // (4 * 64)
    chunks, chunks_down = Chunks(d_model, TAIL_UP).count, Chunks(d_model, TAIL_DOWN).count
    rows = 16 * slots
    x = x.reshape(tokens, d_model)
    kept = jnp.where(slot < slots, expert * slots + slot, -1).astype(F32)
    route = jnp.concatenate([kept.reshape(tokens, top), gate.reshape(tokens, top)], axis=1).T

    dma, vmem, anyw = pltpu.SemaphoreType.DMA, pltpu.VMEM, pl.BlockSpec(memory_space=pl.ANY)
    here = pl.BlockSpec(memory_space=pltpu.VMEM)
    shape = jax.ShapeDtypeStruct
    landing = [shape((chunks, 8, size, DK), BF16) for _, size in PARTS]
    h, hs, g, *_ = pl.pallas_call(
        gather_kernel,
        name="gather_up",
        out_shape=[shape((experts, rows, ff), BF16), shape((tokens, ff), BF16), shape((8, 8 * slots, 2 * tokens), BF16)]
        + landing * 2,
        in_specs=[here, here] + [anyw] * 4,
        out_specs=[anyw] * 9,
        scratch_shapes=[
            vmem((16, 2 * top, tokens), F32),
            vmem((2, 8, 2 * tokens, DK), BF16),
            vmem((experts, rows, DK), BF16),
            vmem((3, DK, 2 * ff), BF16),
            vmem((experts, rows, 2 * ff), F32),
            vmem((tokens, 2 * ff), F32),
            vmem((8, 2, experts * slots, tokens), BF16),
            vmem((2, 8 * slots, 2 * tokens), BF16),
            vmem((8, 64, ff), BF16),
            dma,
            dma((16,)),
            dma((3, chunks)),
            dma((5, 3)),
            dma((3, chunks)),
            dma((3, chunks)),
            dma((3, chunks)),
            dma((2, 3, chunks)),
            dma((2, 2)),
            dma((3,)),
            dma((2,)),
            dma((8,)),
        ],
        compiler_params=pltpu.CompilerParams(has_side_effects=True, vmem_limit_bytes=LIMIT),
    )(x, route, w_gate, w_up, s_gate, s_up)

    def by_part(lead, count):
        return [vmem((lead, count, size, DK), BF16) for _, size in PARTS]

    y = pl.pallas_call(
        scatter_kernel,
        name="down_scatter",
        out_shape=shape((tokens, d_model), BF16),
        in_specs=[anyw] * 5,
        out_specs=here,
        scratch_shapes=[
            vmem((experts, rows, ff), BF16),
            vmem((tokens, ff), BF16),
            vmem((8, 8 * slots, 2 * tokens), BF16),
            vmem((3, ff, DK), BF16),
            vmem((experts, rows, DK), BF16),
            vmem((2, 8, tokens, DK), BF16),
            vmem((2, 8, tokens, DK), BF16),
            vmem((8, tokens, DK), F32),
            vmem((2, 4, tokens, DK), F32),
            vmem((2, 2, tokens, DK), F32),
            vmem((2, tokens, DK), F32),
            *by_part(2, 4), *by_part(2, 2), *by_part(2, 1),
            *by_part(chunks_down, 4), *by_part(chunks_down, 2), *by_part(chunks_down, 1),
            dma((6,)),
            dma((3,)),
            dma((2,)),
            dma((2,)),
            pltpu.SemaphoreType.REGULAR,
            dma((3, 2)),
            dma((3, 2)),
            dma((3, 2)),
            dma((3, chunks_down)),
            dma((3, chunks_down)),
            dma((3, chunks_down)),
        ],
        compiler_params=pltpu.CompilerParams(has_side_effects=True, vmem_limit_bytes=LIMIT),
    )(h, hs, g, w_down, s_down)
    return y.reshape(1, 1, tokens, d_model)


def solution(mesh):
    by_device, by_expert = P("dp", "ep", None, None), P("ep", None, None)
    return jax.shard_map(
        layer,
        mesh=mesh,
        in_specs=(by_device,) * 4 + (by_expert,) * 3 + (P(None, None),) * 3,
        out_specs=by_device,
        check_vma=False,
    )
```

```python
import functools

import jax
import jax.numpy as jnp
from jax import lax
from jax.experimental import pallas as pl
from jax.experimental.pallas import tpu as pltpu
from jax.sharding import PartitionSpec as P

MESH = pl.DeviceIdType.MESH
DK = 512
DN = 256
PARTS = ((0, 96), (96, 80), (176, 80))
LIMIT = 67_000_000
TAIL_UP, TAIL_DOWN = 1, 1
SHARED_FIRST = 1
AHEAD = 2
F32, BF16 = jnp.float32, jnp.bfloat16


class Place:
    def __init__(self):
        self.me = lax.axis_index("ep")
        self.bits = [lax.rem(lax.div(self.me, m), 2) for m in (8, 4, 2)]
        self.core = lax.rem(self.me, 2)
        self.partner = self.me + 1 - 2 * self.core

    def across(self, d):
        ids = [self.me + m * (1 - 2 * b) for m, b in zip((8, 4, 2), self.bits)]
        return ids[0] * lax.div((1 - d) * (2 - d), 2) + ids[1] * (d * (2 - d)) + ids[2] * lax.div(d * (d - 1), 2)

    def chip(self, m):
        ms = (lax.div(m, 4), lax.rem(lax.div(m, 2), 2), lax.rem(m, 2))
        x, y, z = (b + s * (1 - 2 * b) for b, s in zip(self.bits, ms))
        return ((x * 2 + y) * 2 + z) * 2


def turn(o, i):
    return lax.rem(o + i, 3)


def chip_at(o, pos):
    m = 0
    for i in range(3):
        if pos >> i & 1:
            d = turn(o, i)
            m = m + 4 - 2 * d + lax.div(d * (d - 1), 2)
    return m


def cols(k, width):
    return pl.ds(pl.multiple_of(k * width, width), width)


class Chunks:
    def __init__(self, d_model, tail):
        self.count = 1 + (d_model - (1 + tail) * DN) // DK + tail
        self.tail = self.count - tail

    def width(self, k):
        return DK if 0 < k < self.tail else DN

    def of(self, k, width):
        if isinstance(k, int):
            start = sum(self.width(i) for i in range(k))
        else:
            started = lax.div(k + self.count - 1, self.count)
            late = (k - self.tail) * lax.div(k, self.tail + 1)
            start = k * DK - (DK - DN) * (started + late)
        return pl.ds(pl.multiple_of(start, DN), width)

    def when(self, cond, k, work):
        narrow = jnp.logical_or(k == 0, jnp.logical_and(k >= self.tail, k < self.count))
        wide = jnp.logical_and(k > 0, k < self.tail)
        pl.when(jnp.logical_and(cond, narrow))(lambda: work(k, DN))
        pl.when(jnp.logical_and(cond, wide))(lambda: work(k, DK))


def gather_kernel(
    x, route, wg, wu, sg, su,
    h_out, hs_out, g_out, r0, r1, r2, q0, q1, q2,
    rt, xv, z, wbuf, acc, accs, sbuf, gbuf, hbuf,
    route_send, route_recv, fill, send, recv1, recv2, recv3, drecv, load, wsem, gsem, hsem,
):
    at = Place()
    me = at.me
    tokens, d_model = x.shape
    part = Chunks(d_model, TAIL_UP)
    chunks = part.count
    experts, slots = 4, 40
    ff = wg.shape[2]
    r, q = (r0, r1, r2), (q0, q1, q2)

    def remote(src, dst, s, v, dev):
        return pltpu.make_async_remote_copy(
            src_ref=src, dst_ref=dst, send_sem=s, recv_sem=v, device_id={"ep": dev}, device_id_type=MESH
        )

    def first(k, w, p):
        row, size = PARTS[p]
        src, dst = x.at[pl.ds(row, size), part.of(k, w)], r[p].at[k, 1, :, pl.ds(0, w)]
        return remote(src, dst, send.at[0, p], recv1.at[p, k], at.across(turn(k, p)))

    def onward(k, w, p, i):
        n = 2 << i
        src, dst = r[p].at[k, pl.ds(0, n), :, pl.ds(0, w)], r[p].at[k, pl.ds(n, n), :, pl.ds(0, w)]
        return remote(src, dst, send.at[1 + i, p], (recv2, recv3)[i].at[p, k], at.across(turn(k, p + 1 + i)))

    def beside(k, w, p, i):
        half = pl.ds(4 * i, 4)
        src, dst = r[p].at[k, half, :, pl.ds(0, w)], q[p].at[k, half, :, pl.ds(0, w)]
        return remote(src, dst, send.at[3 + i, p], drecv.at[i, p, k], at.partner)

    def filled(k, w, p):
        row, size = PARTS[p]
        return pltpu.make_async_copy(
            x.at[pl.ds(row, size), part.of(k, w)], r[p].at[k, 0, :, pl.ds(0, w)], fill.at[p, k]
        )

    def weights(i):
        slot = lax.rem(i, 3)

        def fetch(gate, up, k, w):
            rows = part.of(k, w)
            for ref, start in ((gate, 0), (up, ff)):
                dst = wbuf.at[slot, pl.ds(0, w), pl.ds(start, ff)]
                pltpu.make_async_copy(ref.at[rows], dst, wsem.at[slot]).start()

        def common(k):
            part.when(True, k, lambda k, w: fetch(sg, su, k, w))

        def routed(e, k):
            part.when(True, k, lambda k, w: fetch(wg.at[e], wu.at[e], k, w))

        rest = i - chunks
        pl.when(rest < 0)(lambda: common(i))
        pl.when(rest >= 0)(lambda: routed(lax.rem(rest, 4), lax.div(rest, 4)))

    def weights_ready(i, w):
        slot = lax.rem(i, 3)
        rows = wbuf.at[slot, pl.ds(0, w)]
        pltpu.make_async_copy(rows, rows, wsem.at[slot]).wait()
        weights(i + 2)
        return slot

    def load_rows(k, w, src, core, i):
        slot = lax.rem(k, 2)
        for p, (row, size) in enumerate(PARTS):
            o = turn(k, p)
            for pos in range(8):
                rows = pl.ds(pl.multiple_of(core * tokens + row, 16), size)
                dst = xv.at[slot, chip_at(o, pos), rows, pl.ds(0, w)]
                pltpu.make_async_copy(src[p].at[k, pos, :, pl.ds(0, w)], dst, load.at[slot, i]).start()

    def rows_ready(k, w, i):
        slot = lax.rem(k, 2)
        half = xv.at[slot, :, pl.ds(0, tokens), pl.ds(0, w)]
        pltpu.make_async_copy(half, half, load.at[slot, i]).wait()

    def begin(k, w):
        for p in range(3):
            first(k, w, p).start()

    def build(m):
        base = at.chip(m)
        row = lax.broadcasted_iota(jnp.int32, (slots, tokens), 0)
        none = jnp.zeros((slots, tokens), F32)

        slot = lax.rem(m, 2)

        @pl.when(m >= 2)
        def _():
            pltpu.make_async_copy(gbuf.at[slot], g_out.at[m - 2], gsem.at[slot]).wait()

        for c in range(2):
            table = rt[base + c]
            hits = []
            for e in range(experts):
                want = (row + (me * experts + e) * slots).astype(F32)
                s, g = none, none
                for j in range(8):
                    hit = want == table[j : j + 1]
                    s = jnp.where(hit, 1.0, s)
                    g = jnp.where(hit, table[8 + j : 9 + j], g)
                hits.append(s)
                both = jnp.concatenate([g, none] if c == 0 else [none, g], axis=0)
                gbuf[slot, e * 80 : (e + 1) * 80, c * tokens : (c + 1) * tokens] = both.astype(BF16)
            sbuf[m, c] = jnp.concatenate(hits, axis=0).astype(BF16)
        pltpu.make_async_copy(gbuf.at[slot], g_out.at[m], gsem.at[slot]).start()

    def accumulate(ref, k, w, a, b):
        if w == DN:

            @pl.when(k == 0)
            def _():
                ref[...] = jnp.dot(a[...], b[...], preferred_element_type=F32)

            @pl.when(k > 0)
            def _():
                ref[...] += jnp.dot(a[...], b[...], preferred_element_type=F32)
        else:
            ref[...] += jnp.dot(a[...], b[...], preferred_element_type=F32)

    def shared(i, w):
        slot = weights_ready(i, w)
        accumulate(accs, i, w, x.at[:, part.of(i, w)], wbuf.at[slot, pl.ds(0, w)])

    def hidden(src, dst, i, rows):
        slot = lax.rem(i, 8)

        @pl.when(i >= 8)
        def _():
            pltpu.make_async_copy(hbuf.at[slot], dst, hsem.at[slot]).wait()

        a = src[rows, pl.ds(0, ff)]
        hbuf[slot] = (a * jax.nn.sigmoid(a) * src[rows, pl.ds(ff, ff)]).astype(BF16)
        pltpu.make_async_copy(hbuf.at[slot], dst, hsem.at[slot]).start()

    def hidden_shared():
        def one(i, _):
            rows = pl.ds(pl.multiple_of(i * 64, 64), 64)
            hidden(accs, hs_out.at[rows], i, rows)
            return 0

        lax.fori_loop(0, tokens // 64, one, 0)

    def hidden_routed(e):
        def one(i, _):
            rows = pl.ds(pl.multiple_of(i * 64, 64), 64)
            hidden(acc.at[e], h_out.at[e, rows], tokens // 64 + 10 * e + i, rows)
            return 0

        lax.fori_loop(0, 10, one, 0)

    def gathered(k, w):
        for p in range(3):
            onward(k, w, p, 1).wait_recv()
            beside(k, w, p, 1).start()
        load_rows(k, w, r, at.core, 0)

    def exchanged(k, w):
        for p in range(3):
            beside(k, w, p, 0).wait_recv()
            beside(k, w, p, 1).wait_recv()
        load_rows(k, w, q, 1 - at.core, 1)

    def compute(k, w):
        slot = lax.rem(k, 2)
        rows_ready(k, w, 0)
        rows_ready(k, w, 1)
        for m in range(8):
            d = [
                jnp.dot(sbuf[m, c], xv[slot, m, c * tokens : (c + 1) * tokens, :w], preferred_element_type=F32)
                for c in range(2)
            ]
            for e in range(experts):
                mine = [v[e * slots : (e + 1) * slots] for v in d]
                z[e, m * 80 : (m + 1) * 80, :w] = jnp.concatenate(mine, axis=0).astype(BF16)

        def expert(e, _):
            part.when(e == 1, k + 2, third)
            part.when(e == 2, k + 1, gathered)
            part.when(e == 3, k + 1, exchanged)
            wslot = weights_ready(chunks + 4 * k + e, w)
            accumulate(acc.at[e], k, w, z.at[e, :, pl.ds(0, w)], wbuf.at[wslot, pl.ds(0, w)])
            if w == DN:
                pl.when(k == chunks - 1)(lambda: hidden_routed(e))
            return 0

        lax.fori_loop(0, experts, expert, 0)

    def second(k, w):
        for p in range(3):
            filled(k, w, p).wait()
            first(k, w, p).wait_recv()
            onward(k, w, p, 0).start()

    def third(k, w):
        for p in range(3):
            onward(k, w, p, 0).wait_recv()
            onward(k, w, p, 1).start()
            beside(k, w, p, 0).start()

    def tables():
        for j in range(1, 16):
            b = lax.rem(me + j, 16)
            remote(route, rt.at[b], route_send, route_recv.at[b], b).wait_recv()

        def one(m, _):
            build(m)
            return 0

        lax.fori_loop(0, 8, one, 0)
        for slot in range(2):
            pltpu.make_async_copy(gbuf.at[slot], g_out.at[slot], gsem.at[slot]).wait()

    def shared_between(lo, hi):
        def one(i, _):
            part.when(True, i, shared)
            return 0

        lax.fori_loop(lo, hi, one, 0)

    def step(s, _):
        pl.when(s == 0)(lambda: shared_between(SHARED_FIRST, 3))
        part.when(s == 2, s - 1, third)
        part.when(True, s, second)
        part.when(True, s + AHEAD, begin)
        pl.when(s == 1)(lambda: shared_between(3, 6))
        part.when(s == 1, s - 1, third)
        pl.when(s == 1)(tables)
        pl.when(s == 2)(lambda: shared_between(6, chunks))
        part.when(s == 2, s - 2, gathered)
        part.when(s == 2, s - 2, exchanged)
        part.when(True, s - 3, compute)
        pl.when(s == 3)(hidden_shared)
        return 0

    entry = pltpu.get_barrier_semaphore()
    for j in range(1, 16):
        pl.semaphore_signal(entry, inc=1, device_id={"ep": lax.rem(me + j, 16)}, device_id_type=MESH)
    weights(0)
    weights(1)
    for k in range(chunks):
        for p in range(3):
            filled(k, part.width(k), p).start()
    rt[me] = route[...]
    shared_between(0, SHARED_FIRST)
    pl.semaphore_wait(entry, 15)
    for k in range(AHEAD):
        begin(k, part.width(k))
    for j in range(1, 16):
        dev = lax.rem(me + j, 16)
        remote(route, rt.at[me], route_send, route_recv.at[me], dev).start()

    lax.fori_loop(0, chunks + 3, step, 0)

    for slot in range(8):
        pltpu.make_async_copy(hbuf.at[slot], hs_out.at[pl.ds(0, 64)], hsem.at[slot]).wait()

    remote(rt.at[pl.ds(0, 15)], rt.at[pl.ds(0, 15)], route_send, route_recv.at[0], at.partner).wait_send()
    for p in range(3):
        for i, rows in enumerate((pl.ds(0, 1), pl.ds(0, 2), pl.ds(0, 4), pl.ds(0, 4), pl.ds(4, 4))):
            sent = r[p].at[pl.ds(0, d_model // DK), rows]
            remote(sent, sent, send.at[i, p], recv1.at[p, 0], at.partner).wait_send()


def scatter_kernel(
    h, hs, g, wd, sd,
    y,
    hv, hsv, gv, wbuf, o, dsend, dland, acc8, acc4, acc2, acc1,
    as0, as1, as2, bs0, bs1, bs2, cs0, cs1, cs2,
    al0, al1, al2, bl0, bl1, bl2, cl0, cl1, cl2,
    start_sem, wsem, dsend_sem, drecv, free, asend_sem, bsend_sem, csend_sem, arecv, brecv, crecv,
):
    at = Place()
    tokens, d_model = y.shape
    part = Chunks(d_model, TAIL_DOWN)
    chunks = part.count
    experts = h.shape[0]
    ff = h.shape[2]
    a_send, b_send, c_send = (as0, as1, as2), (bs0, bs1, bs2), (cs0, cs1, cs2)
    a_land, b_land, c_land = (al0, al1, al2), (bl0, bl1, bl2), (cl0, cl1, cl2)

    def remote(src, dst, s, v, dev):
        return pltpu.make_async_remote_copy(
            src_ref=src, dst_ref=dst, send_sem=s, recv_sem=v, device_id={"ep": dev}, device_id_type=MESH
        )

    def beside(k, w):
        slot = lax.rem(k, 2)
        src, dst = dsend.at[slot, :, :, pl.ds(0, w)], dland.at[slot, :, :, pl.ds(0, w)]
        return remote(src, dst, dsend_sem.at[slot], drecv.at[slot], at.partner)

    def hop(stage, k, w, p):
        slot = lax.rem(k, 2)
        src, dst = (a_send, b_send, c_send)[stage][p], (a_land, b_land, c_land)[stage][p]
        sems, lands = (asend_sem, bsend_sem, csend_sem)[stage], (arecv, brecv, crecv)[stage]
        src, dst = src.at[slot, :, :, pl.ds(0, w)], dst.at[k, :, :, pl.ds(0, w)]
        return remote(src, dst, sems.at[p, slot], lands.at[p, k], at.across(turn(k, p + 2 - stage)))

    def weights(i):
        slot = lax.rem(i, 3)
        e = lax.rem(i, 5)

        def fetch(k, w):
            dst = wbuf.at[slot, :, pl.ds(0, w)]
            pl.when(e < 4)(lambda: pltpu.make_async_copy(wd.at[e, :, part.of(k, w)], dst, wsem.at[slot]).start())
            pl.when(e == 4)(lambda: pltpu.make_async_copy(sd.at[:, part.of(k, w)], dst, wsem.at[slot]).start())

        part.when(True, lax.div(i, 5), fetch)

    def weights_ready(i, w):
        slot = lax.rem(i, 3)
        columns = wbuf.at[slot, :, pl.ds(0, w)]
        pltpu.make_async_copy(columns, columns, wsem.at[slot]).wait()
        weights(i + 2)
        return slot

    entry = pltpu.get_barrier_semaphore()
    for peer in (at.partner, *(at.across(d) for d in range(3))):
        pl.semaphore_signal(entry, inc=1, device_id={"ep": peer}, device_id_type=MESH)

    def hidden(e):
        return pltpu.make_async_copy(h.at[e], hv.at[e], start_sem.at[e])

    common = pltpu.make_async_copy(hs, hsv, start_sem.at[4])
    gates = pltpu.make_async_copy(g, gv, start_sem.at[5])
    hidden(0).start()
    weights(0)
    hidden(1).start()
    weights(1)
    pl.semaphore_wait(entry, 4)

    def compute(k, w):
        slot = lax.rem(k, 2)

        def expert(e, _):
            pl.when(k == 0)(lambda: hidden(e).wait())
            wslot = weights_ready(5 * k + e, w)

            @pl.when(jnp.logical_and(k == 0, e == 0))
            def _():
                for copy in (hidden(2), hidden(3), gates, common):
                    copy.start()

            o[e, :, :w] = jnp.dot(hv[e], wbuf[wslot, :, :w], preferred_element_type=F32).astype(BF16)
            return 0

        lax.fori_loop(0, experts, expert, 0)

        @pl.when(k == 0)
        def _():
            gates.wait()
            common.wait()

        sent(k, lambda v: beside(k, v).wait_send())

        def combine(m, core):
            rows = o[:, m * 80 : (m + 1) * 80, :w].reshape(4 * 80, w)
            return lax.dot_general(gv[m, :, cols(core, 256)], rows, (((0,), (0,)), ((), ())), preferred_element_type=F32)

        for m in range(8):
            dsend[slot, m, :, :w] = combine(m, 1 - at.core).astype(BF16)

        @pl.when(k >= 2)
        def _():
            pl.semaphore_wait(free, 1)

        beside(k, w).start()
        for m in range(8):
            acc8[m, :, :w] = combine(m, at.core)
        wslot = weights_ready(5 * k + 4, w)
        acc8[0, :, :w] += jnp.dot(hsv[...], wbuf[wslot, :, :w], preferred_element_type=F32)

    def sent(k, wait):
        narrow = jnp.logical_or(k == 2, k - 2 >= part.tail)
        pl.when(narrow)(lambda: wait(DN))
        pl.when(jnp.logical_and(k > 2, k - 2 < part.tail))(lambda: wait(DK))

    def first(k, w):
        slot = lax.rem(k, 2)
        beside(k, w).wait_recv()
        for p, (row, size) in enumerate(PARTS):
            sent(k, lambda v: hop(0, k, v, p).wait_send())
            for pos in range(7, -1, -1):
                m = chip_at(turn(k, p), pos)
                v = acc8[m, row : row + size, :w] + dland[slot, m, row : row + size, :w].astype(F32)
                if pos >= 4:
                    a_send[p][slot, pos - 4, :, :w] = v.astype(BF16)
                else:
                    acc4[slot, pos, row : row + size, :w] = v
                if pos == 4:
                    hop(0, k, w, p).start()

        @pl.when(k + 2 < chunks)
        def _():
            pl.semaphore_signal(free, inc=1, device_id={"ep": at.partner}, device_id_type=MESH)

    def second(k, w):
        slot = lax.rem(k, 2)
        for p, (row, size) in enumerate(PARTS):
            hop(0, k, w, p).wait_recv()
            sent(k, lambda v: hop(1, k, v, p).wait_send())
            for pos in range(3, -1, -1):
                v = acc4[slot, pos, row : row + size, :w] + a_land[p][k, pos, :, :w].astype(F32)
                if pos >= 2:
                    b_send[p][slot, pos - 2, :, :w] = v.astype(BF16)
                else:
                    acc2[slot, pos, row : row + size, :w] = v
                if pos == 2:
                    hop(1, k, w, p).start()

    def third(k, w):
        slot = lax.rem(k, 2)
        for p, (row, size) in enumerate(PARTS):
            hop(1, k, w, p).wait_recv()
            sent(k, lambda v: hop(2, k, v, p).wait_send())
            for pos in (1, 0):
                v = acc2[slot, pos, row : row + size, :w] + b_land[p][k, pos, :, :w].astype(F32)
                if pos == 1:
                    c_send[p][slot, 0, :, :w] = v.astype(BF16)
                    hop(2, k, w, p).start()
                else:
                    acc1[slot, row : row + size, :w] = v

    def last(k, w):
        slot = lax.rem(k, 2)
        for p, (row, size) in enumerate(PARTS):
            hop(2, k, w, p).wait_recv()
            out = acc1[slot, row : row + size, :w] + c_land[p][k, 0, :, :w].astype(F32)
            y[row : row + size, part.of(k, w)] = out.astype(BF16)

    def step(s, _):
        for stage, work in ((1, first), (0, compute), (2, second), (3, third), (4, last)):
            part.when(True, s - stage, work)
        return 0

    lax.fori_loop(0, chunks + 4, step, 0)
    for k, w in ((chunks - 2, part.width(chunks - 2)), (chunks - 1, DN)):
        beside(k, w).wait_send()
        for stage in range(3):
            for p in range(3):
                hop(stage, k, w, p).wait_send()


def layer(x, expert, slot, gate, w_gate, w_up, w_down, s_gate, s_up, s_down):
    tokens, d_model = x.shape[2:]
    top = expert.shape[3]
    experts, _, ff = w_gate.shape
    slots = 5 * tokens * top // (4 * 64)
    chunks, chunks_down = Chunks(d_model, TAIL_UP).count, Chunks(d_model, TAIL_DOWN).count
    rows = 16 * slots
    x = x.reshape(tokens, d_model)
    kept = jnp.where(slot < slots, expert * slots + slot, -1).astype(F32)
    route = jnp.concatenate([kept.reshape(tokens, top), gate.reshape(tokens, top)], axis=1).T

    dma, vmem, anyw = pltpu.SemaphoreType.DMA, pltpu.VMEM, pl.BlockSpec(memory_space=pl.ANY)
    here = pl.BlockSpec(memory_space=pltpu.VMEM)
    shape = jax.ShapeDtypeStruct
    landing = [shape((chunks, 8, size, DK), BF16) for _, size in PARTS]
    h, hs, g, *_ = pl.pallas_call(
        gather_kernel,
        name="gather_up",
        out_shape=[shape((experts, rows, ff), BF16), shape((tokens, ff), BF16), shape((8, 8 * slots, 2 * tokens), BF16)]
        + landing * 2,
        in_specs=[here, here] + [anyw] * 4,
        out_specs=[anyw] * 9,
        scratch_shapes=[
            vmem((16, 2 * top, tokens), F32),
            vmem((2, 8, 2 * tokens, DK), BF16),
            vmem((experts, rows, DK), BF16),
            vmem((3, DK, 2 * ff), BF16),
            vmem((experts, rows, 2 * ff), F32),
            vmem((tokens, 2 * ff), F32),
            vmem((8, 2, experts * slots, tokens), BF16),
            vmem((2, 8 * slots, 2 * tokens), BF16),
            vmem((8, 64, ff), BF16),
            dma,
            dma((16,)),
            dma((3, chunks)),
            dma((5, 3)),
            dma((3, chunks)),
            dma((3, chunks)),
            dma((3, chunks)),
            dma((2, 3, chunks)),
            dma((2, 2)),
            dma((3,)),
            dma((2,)),
            dma((8,)),
        ],
        compiler_params=pltpu.CompilerParams(collective_id=1, has_side_effects=True, vmem_limit_bytes=LIMIT),
    )(x, route, w_gate, w_up, s_gate, s_up)

    def by_part(lead, count):
        return [vmem((lead, count, size, DK), BF16) for _, size in PARTS]

    y = pl.pallas_call(
        scatter_kernel,
        name="down_scatter",
        out_shape=shape((tokens, d_model), BF16),
        in_specs=[anyw] * 5,
        out_specs=here,
        scratch_shapes=[
            vmem((experts, rows, ff), BF16),
            vmem((tokens, ff), BF16),
            vmem((8, 8 * slots, 2 * tokens), BF16),
            vmem((3, ff, DK), BF16),
            vmem((experts, rows, DK), BF16),
            vmem((2, 8, tokens, DK), BF16),
            vmem((2, 8, tokens, DK), BF16),
            vmem((8, tokens, DK), F32),
            vmem((2, 4, tokens, DK), F32),
            vmem((2, 2, tokens, DK), F32),
            vmem((2, tokens, DK), F32),
            *by_part(2, 4), *by_part(2, 2), *by_part(2, 1),
            *by_part(chunks_down, 4), *by_part(chunks_down, 2), *by_part(chunks_down, 1),
            dma((6,)),
            dma((3,)),
            dma((2,)),
            dma((2,)),
            pltpu.SemaphoreType.REGULAR,
            dma((3, 2)),
            dma((3, 2)),
            dma((3, 2)),
            dma((3, chunks_down)),
            dma((3, chunks_down)),
            dma((3, chunks_down)),
        ],
        compiler_params=pltpu.CompilerParams(collective_id=0, has_side_effects=True, vmem_limit_bytes=LIMIT),
    )(h, hs, g, w_down, s_down)
    return y.reshape(1, 1, tokens, d_model)


def solution(mesh):
    by_device, by_expert = P("dp", "ep", None, None), P("ep", None, None)
    return jax.shard_map(
        layer,
        mesh=mesh,
        in_specs=(by_device,) * 4 + (by_expert,) * 3 + (P(None, None),) * 3,
        out_specs=by_device,
        check_vma=False,
    )
```

```python
import functools

import jax
import jax.numpy as jnp
from jax import lax
from jax.experimental import pallas as pl
from jax.experimental.pallas import tpu as pltpu
from jax.sharding import PartitionSpec as P

MESH = pl.DeviceIdType.MESH
DK = 512
DN = 256
PARTS = ((0, 96), (96, 80), (176, 80))
LIMIT = 67_000_000
TAIL_UP, TAIL_DOWN = 1, 1
SHARED_FIRST = 1
AHEAD = 2
F32, BF16 = jnp.float32, jnp.bfloat16


class Place:
    def __init__(self):
        self.me = lax.axis_index("ep")
        self.bits = [lax.rem(lax.div(self.me, m), 2) for m in (8, 4, 2)]
        self.core = lax.rem(self.me, 2)
        self.partner = self.me + 1 - 2 * self.core

    def across(self, d):
        ids = [self.me + m * (1 - 2 * b) for m, b in zip((8, 4, 2), self.bits)]
        return ids[0] * lax.div((1 - d) * (2 - d), 2) + ids[1] * (d * (2 - d)) + ids[2] * lax.div(d * (d - 1), 2)

    def chip(self, m):
        ms = (lax.div(m, 4), lax.rem(lax.div(m, 2), 2), lax.rem(m, 2))
        x, y, z = (b + s * (1 - 2 * b) for b, s in zip(self.bits, ms))
        return ((x * 2 + y) * 2 + z) * 2


def turn(o, i):
    return lax.rem(o + i, 3)


def chip_at(o, pos):
    m = 0
    for i in range(3):
        if pos >> i & 1:
            d = turn(o, i)
            m = m + 4 - 2 * d + lax.div(d * (d - 1), 2)
    return m


def cols(k, width):
    return pl.ds(pl.multiple_of(k * width, width), width)


class Chunks:
    def __init__(self, d_model, tail):
        self.count = 1 + (d_model - (1 + tail) * DN) // DK + tail
        self.tail = self.count - tail

    def width(self, k):
        return DK if 0 < k < self.tail else DN

    def of(self, k, width):
        if isinstance(k, int):
            start = sum(self.width(i) for i in range(k))
        else:
            started = lax.div(k + self.count - 1, self.count)
            late = (k - self.tail) * lax.div(k, self.tail + 1)
            start = k * DK - (DK - DN) * (started + late)
        return pl.ds(pl.multiple_of(start, DN), width)

    def when(self, cond, k, work):
        narrow = jnp.logical_or(k == 0, jnp.logical_and(k >= self.tail, k < self.count))
        wide = jnp.logical_and(k > 0, k < self.tail)
        pl.when(jnp.logical_and(cond, narrow))(lambda: work(k, DN))
        pl.when(jnp.logical_and(cond, wide))(lambda: work(k, DK))


def gather_kernel(
    x, route, wg, wu, sg, su,
    h_out, hs_out, g_out, r0, r1, r2, q0, q1, q2,
    rt, xv, z, wbuf, acc, accs, sbuf, gbuf, hbuf,
    route_send, route_recv, fill, send, recv1, recv2, recv3, drecv, load, wsem, gsem, hsem,
):
    at = Place()
    me = at.me
    tokens, d_model = x.shape
    part = Chunks(d_model, TAIL_UP)
    chunks = part.count
    experts, slots = 4, 40
    ff = wg.shape[2]
    r, q = (r0, r1, r2), (q0, q1, q2)

    def remote(src, dst, s, v, dev):
        return pltpu.make_async_remote_copy(
            src_ref=src, dst_ref=dst, send_sem=s, recv_sem=v, device_id={"ep": dev}, device_id_type=MESH
        )

    def first(k, w, p):
        row, size = PARTS[p]
        src, dst = x.at[pl.ds(row, size), part.of(k, w)], r[p].at[k, 1, :, pl.ds(0, w)]
        return remote(src, dst, send.at[0, p], recv1.at[p, k], at.across(turn(k, p)))

    def onward(k, w, p, i):
        n = 2 << i
        src, dst = r[p].at[k, pl.ds(0, n), :, pl.ds(0, w)], r[p].at[k, pl.ds(n, n), :, pl.ds(0, w)]
        return remote(src, dst, send.at[1 + i, p], (recv2, recv3)[i].at[p, k], at.across(turn(k, p + 1 + i)))

    def beside(k, w, p, i):
        half = pl.ds(4 * i, 4)
        src, dst = r[p].at[k, half, :, pl.ds(0, w)], q[p].at[k, half, :, pl.ds(0, w)]
        return remote(src, dst, send.at[3 + i, p], drecv.at[i, p, k], at.partner)

    def filled(k, w, p):
        row, size = PARTS[p]
        return pltpu.make_async_copy(
            x.at[pl.ds(row, size), part.of(k, w)], r[p].at[k, 0, :, pl.ds(0, w)], fill.at[p, k]
        )

    def weights(i):
        slot = lax.rem(i, 3)

        def fetch(gate, up, k, w):
            rows = part.of(k, w)
            for ref, start in ((gate, 0), (up, ff)):
                dst = wbuf.at[slot, pl.ds(0, w), pl.ds(start, ff)]
                pltpu.make_async_copy(ref.at[rows], dst, wsem.at[slot]).start()

        def common(k):
            part.when(True, k, lambda k, w: fetch(sg, su, k, w))

        def routed(e, k):
            part.when(True, k, lambda k, w: fetch(wg.at[e], wu.at[e], k, w))

        rest = i - chunks
        pl.when(rest < 0)(lambda: common(i))
        pl.when(rest >= 0)(lambda: routed(lax.rem(rest, 4), lax.div(rest, 4)))

    def weights_ready(i, w):
        slot = lax.rem(i, 3)
        rows = wbuf.at[slot, pl.ds(0, w)]
        pltpu.make_async_copy(rows, rows, wsem.at[slot]).wait()
        weights(i + 2)
        return slot

    def load_rows(k, w, src, core, i):
        slot = lax.rem(k, 2)
        for p, (row, size) in enumerate(PARTS):
            o = turn(k, p)
            for pos in range(8):
                rows = pl.ds(pl.multiple_of(core * tokens + row, 16), size)
                dst = xv.at[slot, chip_at(o, pos), rows, pl.ds(0, w)]
                pltpu.make_async_copy(src[p].at[k, pos, :, pl.ds(0, w)], dst, load.at[slot, i]).start()

    def rows_ready(k, w, i):
        slot = lax.rem(k, 2)
        half = xv.at[slot, :, pl.ds(0, tokens), pl.ds(0, w)]
        pltpu.make_async_copy(half, half, load.at[slot, i]).wait()

    def begin(k, w):
        for p in range(3):
            first(k, w, p).start()

    def build(m):
        base = at.chip(m)
        row = lax.broadcasted_iota(jnp.int32, (slots, tokens), 0)
        none = jnp.zeros((slots, tokens), F32)

        slot = lax.rem(m, 2)

        @pl.when(m >= 2)
        def _():
            pltpu.make_async_copy(gbuf.at[slot], g_out.at[m - 2], gsem.at[slot]).wait()

        for c in range(2):
            table = rt[base + c]
            hits = []
            for e in range(experts):
                want = (row + (me * experts + e) * slots).astype(F32)
                s, g = none, none
                for j in range(8):
                    hit = want == table[j : j + 1]
                    s = jnp.where(hit, 1.0, s)
                    g = jnp.where(hit, table[8 + j : 9 + j], g)
                hits.append(s)
                both = jnp.concatenate([g, none] if c == 0 else [none, g], axis=0)
                gbuf[slot, e * 80 : (e + 1) * 80, c * tokens : (c + 1) * tokens] = both.astype(BF16)
            sbuf[m, c] = jnp.concatenate(hits, axis=0).astype(BF16)
        pltpu.make_async_copy(gbuf.at[slot], g_out.at[m], gsem.at[slot]).start()

    def accumulate(ref, k, w, a, b):
        if w == DN:

            @pl.when(k == 0)
            def _():
                ref[...] = jnp.dot(a[...], b[...], preferred_element_type=F32)

            @pl.when(k > 0)
            def _():
                ref[...] += jnp.dot(a[...], b[...], preferred_element_type=F32)
        else:
            ref[...] += jnp.dot(a[...], b[...], preferred_element_type=F32)

    def shared(i, w):
        slot = weights_ready(i, w)
        accumulate(accs, i, w, x.at[:, part.of(i, w)], wbuf.at[slot, pl.ds(0, w)])

    def hidden(src, dst, i, rows):
        slot = lax.rem(i, 8)

        @pl.when(i >= 8)
        def _():
            pltpu.make_async_copy(hbuf.at[slot], dst, hsem.at[slot]).wait()

        a = src[rows, pl.ds(0, ff)]
        hbuf[slot] = (a * jax.nn.sigmoid(a) * src[rows, pl.ds(ff, ff)]).astype(BF16)
        pltpu.make_async_copy(hbuf.at[slot], dst, hsem.at[slot]).start()

    def hidden_shared():
        def one(i, _):
            rows = pl.ds(pl.multiple_of(i * 64, 64), 64)
            hidden(accs, hs_out.at[rows], i, rows)
            return 0

        lax.fori_loop(0, tokens // 64, one, 0)

    def hidden_routed(e):
        def one(i, _):
            rows = pl.ds(pl.multiple_of(i * 64, 64), 64)
            hidden(acc.at[e], h_out.at[e, rows], tokens // 64 + 10 * e + i, rows)
            return 0

        lax.fori_loop(0, 10, one, 0)

    def gathered(k, w):
        for p in range(3):
            onward(k, w, p, 1).wait_recv()
            beside(k, w, p, 1).start()
        load_rows(k, w, r, at.core, 0)

    def exchanged(k, w):
        for p in range(3):
            beside(k, w, p, 0).wait_recv()
            beside(k, w, p, 1).wait_recv()
        load_rows(k, w, q, 1 - at.core, 1)

    def compute(k, w):
        slot = lax.rem(k, 2)
        rows_ready(k, w, 0)
        rows_ready(k, w, 1)
        for m in range(8):
            d = [
                jnp.dot(sbuf[m, c], xv[slot, m, c * tokens : (c + 1) * tokens, :w], preferred_element_type=F32)
                for c in range(2)
            ]
            for e in range(experts):
                mine = [v[e * slots : (e + 1) * slots] for v in d]
                z[e, m * 80 : (m + 1) * 80, :w] = jnp.concatenate(mine, axis=0).astype(BF16)

        def expert(e, _):
            part.when(e == 1, k + 2, third)
            part.when(e == 2, k + 1, gathered)
            part.when(e == 3, k + 1, exchanged)
            wslot = weights_ready(chunks + 4 * k + e, w)
            accumulate(acc.at[e], k, w, z.at[e, :, pl.ds(0, w)], wbuf.at[wslot, pl.ds(0, w)])
            if w == DN:
                pl.when(k == chunks - 1)(lambda: hidden_routed(e))
            return 0

        lax.fori_loop(0, experts, expert, 0)

    def second(k, w):
        for p in range(3):
            filled(k, w, p).wait()
            first(k, w, p).wait_recv()
            onward(k, w, p, 0).start()

    def third(k, w):
        for p in range(3):
            onward(k, w, p, 0).wait_recv()
            onward(k, w, p, 1).start()
            beside(k, w, p, 0).start()

    def tables():
        for j in range(1, 16):
            b = lax.rem(me + j, 16)
            remote(route, rt.at[b], route_send, route_recv.at[b], b).wait_recv()

        def one(m, _):
            build(m)
            return 0

        lax.fori_loop(0, 8, one, 0)
        for slot in range(2):
            pltpu.make_async_copy(gbuf.at[slot], g_out.at[slot], gsem.at[slot]).wait()

    def shared_between(lo, hi):
        def one(i, _):
            part.when(True, i, shared)
            return 0

        lax.fori_loop(lo, hi, one, 0)

    def send_route():
        for j in range(1, 16):
            dev = lax.rem(me + j, 16)
            remote(route, rt.at[me], route_send, route_recv.at[me], dev).start()

    def step(s, _):
        pl.when(s == 0)(lambda: shared_between(SHARED_FIRST, 3))
        part.when(s == 2, s - 1, third)
        part.when(True, s, second)
        pl.when(s == 0)(send_route)
        part.when(True, s + AHEAD, begin)
        pl.when(s == 1)(lambda: shared_between(3, 6))
        part.when(s == 1, s - 1, third)
        pl.when(s == 1)(tables)
        pl.when(s == 2)(lambda: shared_between(6, chunks))
        part.when(s == 2, s - 2, gathered)
        part.when(s == 2, s - 2, exchanged)
        part.when(True, s - 3, compute)
        pl.when(s == 3)(hidden_shared)
        return 0

    entry = pltpu.get_barrier_semaphore()
    for j in range(1, 16):
        pl.semaphore_signal(entry, inc=1, device_id={"ep": lax.rem(me + j, 16)}, device_id_type=MESH)
    weights(0)
    weights(1)
    for k in range(chunks):
        for p in range(3):
            filled(k, part.width(k), p).start()
    rt[me] = route[...]
    shared_between(0, SHARED_FIRST)
    pl.semaphore_wait(entry, 15)
    for k in range(AHEAD):
        begin(k, part.width(k))

    lax.fori_loop(0, chunks + 3, step, 0)

    for slot in range(8):
        pltpu.make_async_copy(hbuf.at[slot], hs_out.at[pl.ds(0, 64)], hsem.at[slot]).wait()

    remote(rt.at[pl.ds(0, 15)], rt.at[pl.ds(0, 15)], route_send, route_recv.at[0], at.partner).wait_send()
    for p in range(3):
        for i, rows in enumerate((pl.ds(0, 1), pl.ds(0, 2), pl.ds(0, 4), pl.ds(0, 4), pl.ds(4, 4))):
            sent = r[p].at[pl.ds(0, d_model // DK), rows]
            remote(sent, sent, send.at[i, p], recv1.at[p, 0], at.partner).wait_send()


def scatter_kernel(
    h, hs, g, wd, sd,
    y,
    hv, hsv, gv, wbuf, o, dsend, dland, acc8, acc4, acc2, acc1,
    as0, as1, as2, bs0, bs1, bs2, cs0, cs1, cs2,
    al0, al1, al2, bl0, bl1, bl2, cl0, cl1, cl2,
    start_sem, wsem, dsend_sem, drecv, free, asend_sem, bsend_sem, csend_sem, arecv, brecv, crecv,
):
    at = Place()
    tokens, d_model = y.shape
    part = Chunks(d_model, TAIL_DOWN)
    chunks = part.count
    experts = h.shape[0]
    ff = h.shape[2]
    a_send, b_send, c_send = (as0, as1, as2), (bs0, bs1, bs2), (cs0, cs1, cs2)
    a_land, b_land, c_land = (al0, al1, al2), (bl0, bl1, bl2), (cl0, cl1, cl2)

    def remote(src, dst, s, v, dev):
        return pltpu.make_async_remote_copy(
            src_ref=src, dst_ref=dst, send_sem=s, recv_sem=v, device_id={"ep": dev}, device_id_type=MESH
        )

    def beside(k, w):
        slot = lax.rem(k, 2)
        src, dst = dsend.at[slot, :, :, pl.ds(0, w)], dland.at[slot, :, :, pl.ds(0, w)]
        return remote(src, dst, dsend_sem.at[slot], drecv.at[slot], at.partner)

    def hop(stage, k, w, p):
        slot = lax.rem(k, 2)
        src, dst = (a_send, b_send, c_send)[stage][p], (a_land, b_land, c_land)[stage][p]
        sems, lands = (asend_sem, bsend_sem, csend_sem)[stage], (arecv, brecv, crecv)[stage]
        src, dst = src.at[slot, :, :, pl.ds(0, w)], dst.at[k, :, :, pl.ds(0, w)]
        return remote(src, dst, sems.at[p, slot], lands.at[p, k], at.across(turn(k, p + 2 - stage)))

    def weights(i):
        slot = lax.rem(i, 3)
        e = lax.rem(i, 5)

        def fetch(k, w):
            dst = wbuf.at[slot, :, pl.ds(0, w)]
            pl.when(e < 4)(lambda: pltpu.make_async_copy(wd.at[e, :, part.of(k, w)], dst, wsem.at[slot]).start())
            pl.when(e == 4)(lambda: pltpu.make_async_copy(sd.at[:, part.of(k, w)], dst, wsem.at[slot]).start())

        part.when(True, lax.div(i, 5), fetch)

    def weights_ready(i, w):
        slot = lax.rem(i, 3)
        columns = wbuf.at[slot, :, pl.ds(0, w)]
        pltpu.make_async_copy(columns, columns, wsem.at[slot]).wait()
        weights(i + 2)
        return slot

    entry = pltpu.get_barrier_semaphore()
    for peer in (at.partner, *(at.across(d) for d in range(3))):
        pl.semaphore_signal(entry, inc=1, device_id={"ep": peer}, device_id_type=MESH)

    def hidden(e):
        return pltpu.make_async_copy(h.at[e], hv.at[e], start_sem.at[e])

    common = pltpu.make_async_copy(hs, hsv, start_sem.at[4])
    gates = pltpu.make_async_copy(g, gv, start_sem.at[5])
    hidden(0).start()
    weights(0)
    hidden(1).start()
    weights(1)
    pl.semaphore_wait(entry, 4)

    def compute(k, w):
        slot = lax.rem(k, 2)

        def expert(e, _):
            pl.when(k == 0)(lambda: hidden(e).wait())
            wslot = weights_ready(5 * k + e, w)

            @pl.when(jnp.logical_and(k == 0, e == 0))
            def _():
                for copy in (hidden(2), hidden(3), gates, common):
                    copy.start()

            o[e, :, :w] = jnp.dot(hv[e], wbuf[wslot, :, :w], preferred_element_type=F32).astype(BF16)
            return 0

        lax.fori_loop(0, experts, expert, 0)

        @pl.when(k == 0)
        def _():
            gates.wait()
            common.wait()

        sent(k, lambda v: beside(k, v).wait_send())

        def combine(m, core):
            rows = o[:, m * 80 : (m + 1) * 80, :w].reshape(4 * 80, w)
            return lax.dot_general(gv[m, :, cols(core, 256)], rows, (((0,), (0,)), ((), ())), preferred_element_type=F32)

        for m in range(8):
            dsend[slot, m, :, :w] = combine(m, 1 - at.core).astype(BF16)

        @pl.when(k >= 2)
        def _():
            pl.semaphore_wait(free, 1)

        beside(k, w).start()
        for m in range(8):
            acc8[m, :, :w] = combine(m, at.core)
        wslot = weights_ready(5 * k + 4, w)
        acc8[0, :, :w] += jnp.dot(hsv[...], wbuf[wslot, :, :w], preferred_element_type=F32)

    def sent(k, wait):
        narrow = jnp.logical_or(k == 2, k - 2 >= part.tail)
        pl.when(narrow)(lambda: wait(DN))
        pl.when(jnp.logical_and(k > 2, k - 2 < part.tail))(lambda: wait(DK))

    def first(k, w):
        slot = lax.rem(k, 2)
        beside(k, w).wait_recv()
        for p, (row, size) in enumerate(PARTS):
            sent(k, lambda v: hop(0, k, v, p).wait_send())
            for pos in range(7, -1, -1):
                m = chip_at(turn(k, p), pos)
                v = acc8[m, row : row + size, :w] + dland[slot, m, row : row + size, :w].astype(F32)
                if pos >= 4:
                    a_send[p][slot, pos - 4, :, :w] = v.astype(BF16)
                else:
                    acc4[slot, pos, row : row + size, :w] = v
                if pos == 4:
                    hop(0, k, w, p).start()

        @pl.when(k + 2 < chunks)
        def _():
            pl.semaphore_signal(free, inc=1, device_id={"ep": at.partner}, device_id_type=MESH)

    def second(k, w):
        slot = lax.rem(k, 2)
        for p, (row, size) in enumerate(PARTS):
            hop(0, k, w, p).wait_recv()
            sent(k, lambda v: hop(1, k, v, p).wait_send())
            for pos in range(3, -1, -1):
                v = acc4[slot, pos, row : row + size, :w] + a_land[p][k, pos, :, :w].astype(F32)
                if pos >= 2:
                    b_send[p][slot, pos - 2, :, :w] = v.astype(BF16)
                else:
                    acc2[slot, pos, row : row + size, :w] = v
                if pos == 2:
                    hop(1, k, w, p).start()

    def third(k, w):
        slot = lax.rem(k, 2)
        for p, (row, size) in enumerate(PARTS):
            hop(1, k, w, p).wait_recv()
            sent(k, lambda v: hop(2, k, v, p).wait_send())
            for pos in (1, 0):
                v = acc2[slot, pos, row : row + size, :w] + b_land[p][k, pos, :, :w].astype(F32)
                if pos == 1:
                    c_send[p][slot, 0, :, :w] = v.astype(BF16)
                    hop(2, k, w, p).start()
                else:
                    acc1[slot, row : row + size, :w] = v

    def last(k, w):
        slot = lax.rem(k, 2)
        for p, (row, size) in enumerate(PARTS):
            hop(2, k, w, p).wait_recv()
            out = acc1[slot, row : row + size, :w] + c_land[p][k, 0, :, :w].astype(F32)
            y[row : row + size, part.of(k, w)] = out.astype(BF16)

    def step(s, _):
        for stage, work in ((1, first), (0, compute), (2, second), (3, third), (4, last)):
            part.when(True, s - stage, work)
        return 0

    lax.fori_loop(0, chunks + 4, step, 0)
    for k, w in ((chunks - 2, part.width(chunks - 2)), (chunks - 1, DN)):
        beside(k, w).wait_send()
        for stage in range(3):
            for p in range(3):
                hop(stage, k, w, p).wait_send()


def layer(x, expert, slot, gate, w_gate, w_up, w_down, s_gate, s_up, s_down):
    tokens, d_model = x.shape[2:]
    top = expert.shape[3]
    experts, _, ff = w_gate.shape
    slots = 5 * tokens * top // (4 * 64)
    chunks, chunks_down = Chunks(d_model, TAIL_UP).count, Chunks(d_model, TAIL_DOWN).count
    rows = 16 * slots
    x = x.reshape(tokens, d_model)
    kept = jnp.where(slot < slots, expert * slots + slot, -1).astype(F32)
    route = jnp.concatenate([kept.reshape(tokens, top), gate.reshape(tokens, top)], axis=1).T

    dma, vmem, anyw = pltpu.SemaphoreType.DMA, pltpu.VMEM, pl.BlockSpec(memory_space=pl.ANY)
    here = pl.BlockSpec(memory_space=pltpu.VMEM)
    shape = jax.ShapeDtypeStruct
    landing = [shape((chunks, 8, size, DK), BF16) for _, size in PARTS]
    h, hs, g, *_ = pl.pallas_call(
        gather_kernel,
        name="gather_up",
        out_shape=[shape((experts, rows, ff), BF16), shape((tokens, ff), BF16), shape((8, 8 * slots, 2 * tokens), BF16)]
        + landing * 2,
        in_specs=[here, here] + [anyw] * 4,
        out_specs=[anyw] * 9,
        scratch_shapes=[
            vmem((16, 2 * top, tokens), F32),
            vmem((2, 8, 2 * tokens, DK), BF16),
            vmem((experts, rows, DK), BF16),
            vmem((3, DK, 2 * ff), BF16),
            vmem((experts, rows, 2 * ff), F32),
            vmem((tokens, 2 * ff), F32),
            vmem((8, 2, experts * slots, tokens), BF16),
            vmem((2, 8 * slots, 2 * tokens), BF16),
            vmem((8, 64, ff), BF16),
            dma,
            dma((16,)),
            dma((3, chunks)),
            dma((5, 3)),
            dma((3, chunks)),
            dma((3, chunks)),
            dma((3, chunks)),
            dma((2, 3, chunks)),
            dma((2, 2)),
            dma((3,)),
            dma((2,)),
            dma((8,)),
        ],
        compiler_params=pltpu.CompilerParams(collective_id=1, has_side_effects=True, vmem_limit_bytes=LIMIT),
    )(x, route, w_gate, w_up, s_gate, s_up)

    def by_part(lead, count):
        return [vmem((lead, count, size, DK), BF16) for _, size in PARTS]

    y = pl.pallas_call(
        scatter_kernel,
        name="down_scatter",
        out_shape=shape((tokens, d_model), BF16),
        in_specs=[anyw] * 5,
        out_specs=here,
        scratch_shapes=[
            vmem((experts, rows, ff), BF16),
            vmem((tokens, ff), BF16),
            vmem((8, 8 * slots, 2 * tokens), BF16),
            vmem((3, ff, DK), BF16),
            vmem((experts, rows, DK), BF16),
            vmem((2, 8, tokens, DK), BF16),
            vmem((2, 8, tokens, DK), BF16),
            vmem((8, tokens, DK), F32),
            vmem((2, 4, tokens, DK), F32),
            vmem((2, 2, tokens, DK), F32),
            vmem((2, tokens, DK), F32),
            *by_part(2, 4), *by_part(2, 2), *by_part(2, 1),
            *by_part(chunks_down, 4), *by_part(chunks_down, 2), *by_part(chunks_down, 1),
            dma((6,)),
            dma((3,)),
            dma((2,)),
            dma((2,)),
            pltpu.SemaphoreType.REGULAR,
            dma((3, 2)),
            dma((3, 2)),
            dma((3, 2)),
            dma((3, chunks_down)),
            dma((3, chunks_down)),
            dma((3, chunks_down)),
        ],
        compiler_params=pltpu.CompilerParams(collective_id=0, has_side_effects=True, vmem_limit_bytes=LIMIT),
    )(h, hs, g, w_down, s_down)
    return y.reshape(1, 1, tokens, d_model)


def solution(mesh):
    by_device, by_expert = P("dp", "ep", None, None), P("ep", None, None)
    return jax.shard_map(
        layer,
        mesh=mesh,
        in_specs=(by_device,) * 4 + (by_expert,) * 3 + (P(None, None),) * 3,
        out_specs=by_device,
        check_vma=False,
    )
```
